256 devices in a mesh: row: 32 (over y, z), col: 8 (over x, core).
Axes of the slice: x: 4, y: 4, z: 8, core: 2. Of those that a mesh axis runs over, the one named last changes fastest.
Arguments:
- eigvecs: float32 [131072, 1024], P('row', 'col'), may hold values from -6 to 6
- reflectors: float32 [4, 131072, 256], P(None, ('row', 'col'))
- factors: float32 [4, 256, 256], replicated, as said below
Outputs:
- transformed: float32 [131072, 1024], P('row', 'col')
The draws below stay inside these ranges and needn't reach their ends.
Inputs may be any that keep to these rules, and one draw needn't show every extreme that they name: Each factors[k] is upper triangular with a positive diagonal.
All inputs are finite; a program needn't handle non-finite values.
Results may differ from the reference program's by a relative error of at most 0.00012.
Values sent between devices are 32-bit elements; how exact they have to be, the bound alone decides.
A program may use at most 128 MiB of HBM per device.

```python
import jax
import jax.numpy as jnp
from jax import lax

N = 131072
M = 1024
WB = 256
PANELS = 4


def draw_reflectors(key, part):
    scale = (N * WB) ** (-0.25)
    base = jnp.clip(jax.random.normal(key, (PANELS, N, WB), jnp.float32), -6.0, 6.0)
    return base * scale


def draw_factors(key, part):
    diag = jax.random.uniform(key, (PANELS, WB), jnp.float32, 0.5, 1.5)
    off = 0.5 * jnp.clip(jax.random.normal(jax.random.fold_in(key, 3), (PANELS, WB, WB), jnp.float32), -6.0, 6.0) / jnp.sqrt(WB * 1.0)
    upper = jnp.triu(off, 1)
    eye = jnp.eye(WB, dtype=jnp.float32)
    return upper + eye[None, :, :] * diag[:, None, :]


def block_scale(rng, dims, pieces, low, top_value):
    def one(position, parts):
        heights = jax.random.uniform(jax.random.fold_in(jax.random.fold_in(rng, 6), position), (parts,), jnp.float32, low / len(pieces), top_value / len(pieces))
        return jnp.repeat(jnp.exp(heights), dims[position] // parts).reshape((-1,) + (1,) * (len(dims) - position - 1))

    factor_of = one(*pieces[0])
    for cut in pieces[1:]:
        factor_of = factor_of * one(*cut)
    return factor_of


def scatter_about(stream_key, dims, deviation, reach, split=(), kind=jnp.bfloat16):
    array = deviation * jax.random.normal(stream_key, dims, jnp.float32)
    if split:
        array = array * block_scale(stream_key, dims, split, -0.22, 0.18)
    return jnp.clip(array, -reach, reach).astype(kind)


def setup_inputs(seed: int = 0) -> dict:
    splits = jax.random.split(jax.random.key(seed), 4)
    return {
        "eigvecs": scatter_about(splits[0], (N, M), 1.0, 6.0, ((0, 32), (1, 8)), jnp.float32),
        "reflectors": draw_reflectors(jax.random.fold_in(splits[3], 71), 0),
        "factors": draw_factors(jax.random.fold_in(splits[3], 71), 0),
    }


def reference(eigvecs, reflectors, factors):
    field = eigvecs
    for index in range(PANELS):
        vectors = reflectors[index]
        proj = lax.dot_general(vectors, field, (((0,), (0,)), ((), ())), precision=lax.Precision.HIGHEST, preferred_element_type=jnp.float32)
        coeffs = jnp.dot(factors[index], proj, precision=lax.Precision.HIGHEST, preferred_element_type=jnp.float32)
        field = field - jnp.dot(vectors, coeffs, precision=lax.Precision.HIGHEST, preferred_element_type=jnp.float32)
    return field
```

```python
import jax
import jax.numpy as jnp
from jax import lax
from jax.experimental import pallas as pl
from jax.experimental.pallas import tpu as pltpu
from jax.sharding import PartitionSpec as P

MESH = pl.DeviceIdType.MESH
F32 = jnp.float32
BF16 = jnp.bfloat16

NX, NY, NZ, NC = 4, 4, 8, 2
PANELS, WB = 4, 256
ROWS, COLS = 4096, 128
OWN = 512
CHIP = NC * OWN
CH = 4
CW = COLS // CH
CM = NX * CW
ZW = CM // NZ
PAIRS = [(0, 1), (0, 2), (0, 3), (1, 2), (1, 3), (2, 3)]
HALF = len(PAIRS) // NC
HA = 2 * WB
HB = HALF * WB - HA
HAY, HAZ = HA // NY, HA // NY // NZ
HBZ, HBY = HB // NZ, HB // NZ // NY
HX = HAZ + HBY


def split(x):
    high = x.astype(BF16)
    return high, (x - high.astype(F32)).astype(BF16)


def dot3(a, b, dims):
    def one(left, right):
        return lax.dot_general(left, right, (dims, ((), ())), preferred_element_type=F32)

    (ah, al), (bh, bl) = a, b
    return one(ah, bh) + (one(al, bh) + one(ah, bl))


NN = ((1,), (0,))
NT = ((1,), (1,))
TN = ((0,), (0,))


def kernel(
    f_hbm, v_hbm, t_hbm, out_hbm,
    fv, ft, vown, vsib, tv, th, tl, vh, vl, wh, wl, fin, qp, yr, ys, zr, zs, xr, qf, sol, ut, uin,
    gp, gc, gs, ayr, ays, azr, bzr, bzs, byr, gx, gxr, gf, gh, gl,
    lsem, ssem, rsem, csem,
):
    row, col = lax.axis_index("row"), lax.axis_index("col")
    y, z, x, c = row // NZ, row % NZ, col // NC, col % NC

    def device(nx=x, ny=y, nz=z, nc=c):
        return (ny * NZ + nz, nx * NC + nc)

    def along(axis, d):
        if axis == "x":
            pos = lax.rem(x + d, NX)
            return pos, device(nx=pos)
        if axis == "y":
            pos = lax.rem(y + d, NY)
            return pos, device(ny=pos)
        if axis == "z":
            pos = lax.rem(z + d, NZ)
            return pos, device(nz=pos)
        pos = lax.rem(c + d, NC)
        return pos, device(nc=pos)

    sizes = {"x": NX, "y": NY, "z": NZ, "c": NC}
    started = []
    counter = [0]

    def exchange(axis, source, target):
        copies = []
        for d in range(1, sizes[axis]):
            pos, peer = along(axis, d)
            copy = pltpu.make_async_remote_copy(
                src_ref=source(pos), dst_ref=target(d), send_sem=ssem.at[counter[0]], recv_sem=rsem.at[counter[0]],
                device_id=peer, device_id_type=MESH,
            )
            counter[0] += 1
            copy.start()
            copies.append(copy)
        started.extend(copies)
        return copies

    def arrive(copies):
        for copy in copies:
            copy.wait_recv()

    loads = [
        pltpu.make_async_copy(f_hbm, fv, lsem.at[0]),
        pltpu.make_async_copy(v_hbm, vown, lsem.at[1]),
        pltpu.make_async_copy(t_hbm, tv, lsem.at[2]),
    ]
    for load in loads:
        load.start()

    barrier = pltpu.get_barrier_semaphore()
    peers = 0
    for axis in ("x", "y", "z", "c"):
        for d in range(1, sizes[axis]):
            pl.semaphore_signal(barrier, inc=1, device_id=along(axis, d)[1], device_id_type=MESH)
            peers += 1

    loads[0].wait()

    @pl.loop(0, ROWS // 128)
    def _(b):
        at = pl.multiple_of(b * 128, 128)
        ft[:, pl.ds(at, 128)] = fv[pl.ds(at, 128), :].T

    pl.semaphore_wait(barrier, peers)

    def chip_rows(pos):
        return pl.ds(pl.multiple_of(pos * CHIP, CHIP), CHIP)

    def part(pos, size):
        return pl.ds(pl.multiple_of(pos * size, size), size)

    def send_in(h):
        rows = pl.ds(h * CW, CW)
        copies = exchange("x", lambda pos: ft.at[rows, chip_rows(pos)], lambda d: fin.at[h, part(x, CW), :])
        fin[h, part(x, CW), :] = ft[rows, chip_rows(x)]
        return copies

    ins = {0: send_in(0)}
    loads[1].wait()
    sib = exchange("c", lambda pos: v_hbm, lambda d: vsib)
    ins[1] = send_in(1)

    loads[2].wait()
    for k in range(PANELS):
        th[k], tl[k] = split(tv[k])

    def prepare(source, where):
        rows = part(where, OWN)

        @pl.loop(0, PANELS)
        def _(k):
            high, low = split(source[k])
            vh[k, rows, :] = high
            vl[k, rows, :] = low
            w = dot3((high, low), (th[k], tl[k]), NN)
            high, low = split(w)
            wh[k, rows, :] = high
            wl[k, rows, :] = low

    prepare(vown, c)
    mine = part(c, OWN)
    for index, (j, k) in enumerate(PAIRS):
        gp[pl.ds(index * WB, WB), :] = dot3((wh[j, mine, :], wl[j, mine, :]), (vh[k, mine, :], vl[k, mine, :]), TN)

    share = HALF * WB
    gcs = exchange("c", lambda pos: gp.at[part(pos, share), :], lambda d: gc)
    arrive(gcs)
    gs[...] = gp[part(c, share), :] + gc[...]
    ay = exchange("y", lambda pos: gs.at[part(pos, HAY), :], lambda d: ayr.at[d - 1])
    bz = exchange("z", lambda pos: gs.at[pl.ds(pl.multiple_of(HA + pos * HBZ, HBZ), HBZ), :], lambda d: bzr.at[d - 1])

    arrive(sib)
    prepare(vsib, 1 - c)

    def project(h):
        high, low = split(fin[h])

        @pl.loop(0, PANELS)
        def _(k):
            qp[h, k] = dot3((high, low), (vh[k], vl[k]), NN)

    def send_yrs(h):
        return exchange("y", lambda pos: qp.at[h, pos], lambda d: yr.at[h, d - 1])

    def sum_yrs(h):
        ys[h] = (qp[h, y] + yr[h, 0]) + (yr[h, 1] + yr[h, 2])

    def send_zrs(h):
        return exchange("z", lambda pos: ys.at[h, part(pos, ZW), :], lambda d: zr.at[h, d - 1])

    def sum_zrs(h):
        total = ys[h, part(z, ZW), :]
        for d in range(NZ - 1):
            total = total + zr[h, d]
        zs[h] = total

    def send_x(h):
        return exchange("x", lambda pos: zs.at[h], lambda d: xr.at[h, d - 1])

    def sum_x(h):
        qf[h, y, part(z, ZW), :] = (zs[h] + xr[h, 0]) + (xr[h, 1] + xr[h, 2])

    def send_zag(h):
        here = qf.at[h, y, part(z, ZW), :]
        return exchange("z", lambda pos: here, lambda d: here)

    def send_yag(h):
        here = qf.at[h, y]
        return exchange("y", lambda pos: here, lambda d: here)

    def pair(j, k):
        return pl.ds(PAIRS.index((j, k)) * WB, WB)

    def solve(h):
        proj = [qf[h, k] for k in range(PANELS)]
        for j in range(PANELS):
            high, low = split(proj[j])
            sol[h, 0, j] = high
            sol[h, 1, j] = low
            for k in range(j + 1, PANELS):
                proj[k] = proj[k] - dot3((high, low), (gh[pair(j, k), :], gl[pair(j, k), :]), NN)
        ut[h] = jnp.zeros((CM, CHIP), F32)

        @pl.loop(0, PANELS)
        def _(k):
            ut[h] += dot3((sol[h, 0, k], sol[h, 1, k]), (wh[k], wl[k]), NT)

    def send_out(h):
        rows = pl.ds(h * CW, CW)
        copies = exchange("x", lambda pos: ut.at[h, part(pos, CW), :], lambda d: uin.at[rows, chip_rows(x)])
        uin[rows, chip_rows(x)] = ut[h, part(x, CW), :]
        return copies

    def pairs_first():
        arrive(ay)
        ays[...] = (gs[part(y, HAY), :] + ayr[0]) + (ayr[1] + ayr[2])
        arrive(bz)
        total = gs[pl.ds(pl.multiple_of(HA + z * HBZ, HBZ), HBZ), :]
        for d in range(NZ - 1):
            total = total + bzr[d]
        bzs[...] = total
        az = exchange("z", lambda pos: ays.at[part(pos, HAZ), :], lambda d: azr.at[d - 1])
        by = exchange("y", lambda pos: bzs.at[part(pos, HBY), :], lambda d: byr.at[d - 1])
        return az, by

    def pairs_second(az, by):
        arrive(az)
        total = ays[part(z, HAZ), :]
        for d in range(NZ - 1):
            total = total + azr[d]
        gx[pl.ds(0, HAZ), :] = total
        arrive(by)
        gx[pl.ds(HAZ, HBY), :] = (bzs[part(y, HBY), :] + byr[0]) + (byr[1] + byr[2])
        return exchange("x", lambda pos: gx, lambda d: gxr.at[d - 1])

    base = c * share
    spot_a = pl.ds(pl.multiple_of(base + y * HAY + z * HAZ, HAZ), HAZ)
    line_a = pl.ds(pl.multiple_of(base + y * HAY, HAY), HAY)
    spot_b = pl.ds(pl.multiple_of(base + HA + z * HBZ + y * HBY, HBY), HBY)
    line_b = pl.ds(pl.multiple_of(base + HA + z * HBZ, HBZ), HBZ)

    def pairs_third(copies):
        arrive(copies)
        total = (gx[...] + gxr[0]) + (gxr[1] + gxr[2])
        gf[spot_a, :] = total[:HAZ]
        gf[spot_b, :] = total[HAZ:]
        az = exchange("z", lambda pos: gf.at[spot_a, :], lambda d: gf.at[spot_a, :])
        by = exchange("y", lambda pos: gf.at[spot_b, :], lambda d: gf.at[spot_b, :])
        return az, by

    def pairs_fourth(az, by):
        arrive(az)
        arrive(by)
        ay = exchange("y", lambda pos: gf.at[line_a, :], lambda d: gf.at[line_a, :])
        bz = exchange("z", lambda pos: gf.at[line_b, :], lambda d: gf.at[line_b, :])
        return ay, bz

    def pairs_fifth(ay, bz):
        arrive(ay)
        arrive(bz)
        return exchange("c", lambda pos: gf.at[part(c, share), :], lambda d: gf.at[part(c, share), :])

    def pairs_last(copies):
        arrive(copies)
        gh[...], gl[...] = split(gf[...])

    yrs, zrs, xs, zag, yag, outs = {}, {}, {}, {}, {}, {}

    def step_in(h):
        arrive(ins[h])
        if h + 2 < CH:
            ins[h + 2] = send_in(h + 2)
        project(h)
        yrs[h] = send_yrs(h)

    def step_y(h):
        arrive(yrs[h])
        sum_yrs(h)
        zrs[h] = send_zrs(h)

    def step_z(h):
        arrive(zrs[h])
        sum_zrs(h)
        xs[h] = send_x(h)

    def step_x(h):
        arrive(xs[h])
        sum_x(h)
        zag[h] = send_zag(h)

    def step_zag(h):
        arrive(zag[h])
        yag[h] = send_yag(h)

    def step_out(h):
        arrive(yag[h])
        solve(h)
        outs[h] = send_out(h)

    step_in(0)
    first = pairs_first()
    step_in(1)
    step_y(0)
    second = pairs_second(*first)
    step_in(2)
    step_z(0)
    third = pairs_third(second)
    step_y(1)
    step_in(3)
    step_x(0)
    step_z(1)
    fourth = pairs_fourth(*third)
    step_y(2)
    step_zag(0)
    step_x(1)
    step_z(2)
    step_y(3)
    fifth = pairs_fifth(*fourth)
    step_zag(1)
    step_x(2)
    pairs_last(fifth)
    step_out(0)
    step_z(3)
    step_zag(2)
    step_out(1)
    step_x(3)
    step_zag(3)
    step_out(2)
    step_out(3)

    for h in range(CH):
        arrive(outs[h])

    @pl.loop(0, ROWS // 128)
    def _(b):
        at = pl.multiple_of(b * 128, 128)
        fv[pl.ds(at, 128), :] = fv[pl.ds(at, 128), :] - uin[:, pl.ds(at, 128)].T

    for copy in started:
        copy.wait_send()
    store = pltpu.make_async_copy(fv, out_hbm, csem)
    store.start()
    store.wait()


COPIES = NC - 1 + CH * (4 * (NX - 1) - 1 * (NX - 1) + 2 * (NY - 1) + 2 * (NZ - 1)) + 2 * (NC - 1) + 4 * (NY - 1) + 4 * (NZ - 1) + (NX - 1)


def body(eigvecs, reflectors, factors):
    def vm(shape, dtype=F32):
        return pltpu.VMEM(shape, dtype)

    scratch = [
        vm((ROWS, COLS)), vm((COLS, ROWS)), vm((PANELS, OWN, WB)), vm((PANELS, OWN, WB)), vm((PANELS, WB, WB)),
        vm((PANELS, WB, WB), BF16), vm((PANELS, WB, WB), BF16),
        vm((PANELS, CHIP, WB), BF16), vm((PANELS, CHIP, WB), BF16), vm((PANELS, CHIP, WB), BF16), vm((PANELS, CHIP, WB), BF16),
        vm((CH, CM, CHIP)), vm((CH, PANELS, CM, WB)), vm((CH, NY - 1, CM, WB)), vm((CH, CM, WB)),
        vm((CH, NZ - 1, ZW, WB)), vm((CH, ZW, WB)), vm((CH, NX - 1, ZW, WB)), vm((CH, PANELS, CM, WB)),
        vm((CH, 2, PANELS, CM, WB), BF16), vm((CH, CM, CHIP)), vm((COLS, ROWS)),
        vm((len(PAIRS) * WB, WB)), vm((HALF * WB, WB)), vm((HALF * WB, WB)),
        vm((NY - 1, HAY, WB)), vm((HAY, WB)), vm((NZ - 1, HAZ, WB)), vm((NZ - 1, HBZ, WB)), vm((HBZ, WB)), vm((NY - 1, HBY, WB)),
        vm((HX, WB)), vm((NX - 1, HX, WB)), vm((len(PAIRS) * WB, WB)), vm((len(PAIRS) * WB, WB), BF16), vm((len(PAIRS) * WB, WB), BF16),
        pltpu.SemaphoreType.DMA((3,)), pltpu.SemaphoreType.DMA((COPIES,)), pltpu.SemaphoreType.DMA((COPIES,)), pltpu.SemaphoreType.DMA,
    ]
    return pl.pallas_call(
        kernel,
        out_shape=jax.ShapeDtypeStruct((ROWS, COLS), F32),
        in_specs=[pl.BlockSpec(memory_space=pl.ANY)] * 3,
        out_specs=pl.BlockSpec(memory_space=pl.ANY),
        scratch_shapes=scratch,
        compiler_params=pltpu.CompilerParams(collective_id=0, has_side_effects=True, vmem_limit_bytes=63 * 2**20),
        name="back_transform",
    )(eigvecs, reflectors, factors)


def solution(mesh):
    in_specs = (P("row", "col"), P(None, ("row", "col"), None), P())
    return jax.shard_map(body, mesh=mesh, in_specs=in_specs, out_specs=P("row", "col"), check_vma=False)
```

```python
import jax
import jax.numpy as jnp
from jax import lax
from jax.experimental import pallas as pl
from jax.experimental.pallas import tpu as pltpu
from jax.sharding import PartitionSpec as P

MESH = pl.DeviceIdType.MESH
F32 = jnp.float32
BF16 = jnp.bfloat16

SIZES = {"x": 4, "y": 4, "z": 8, "c": 2}
NX, NY, NZ, NC = SIZES.values()
PANELS, WB = 4, 256
ROWS, COLS = 4096, 128
OWN = 512
CHIP = NC * OWN
WIDE = PANELS * WB
CH = 8
CW = COLS // CH
CM = NX * CW
PAIRS = [(0, 1), (0, 2), (0, 3), (1, 2), (1, 3), (2, 3)]
SHARE = len(PAIRS) // NC * WB
HA = 2 * WB
HB = SHARE - HA
AM = HA // NY
BZ, BY = HB // NZ, HB // NZ // NY
A = CH
ORDER = [
    ("gc",), ("next", 1), ("next", 2), ("next", 3), ("next", 4), ("next", 5), ("sib",), ("in", 0), ("in", 1), ("r1", A),
    ("r1", 0), ("b1",), ("in", 3), ("b2",), ("in", 4), ("r1", 1), ("r2", A), ("b3",), ("next", 6), ("x", A), ("in", 2), ("r1", 3),
    ("r1", 4), ("r2", 1), ("b4",), ("a1", A), ("next", 7), ("in", 6), ("r1", 2), ("r2", 3), ("in", 5), ("x", 1), ("r2", 4),
    ("a2", A), ("in", 7), ("x", 4), ("x", 3), ("r1", 6), ("r2", 2), ("r1", 5), ("r2", 0), ("a1", 1), ("pairs",), ("a1", 4),
    ("x", 2), ("r1", 7), ("x", 0), ("fold", 2), ("fold", 1), ("a1", 3), ("fold", 0), ("r2", 6), ("r2", 5), ("out", 1), ("x", 6),
    ("r2", 7), ("a1", 2), ("x", 5), ("out", 4), ("a1", 0), ("out", 3), ("a1", 6), ("x", 7), ("out", 2), ("a1", 5), ("out", 0),
    ("a1", 7), ("out", 6), ("out", 5), ("out", 7),
]


def split(x):
    high = x.astype(BF16)
    return high, (x - high.astype(F32)).astype(BF16)


def dot3(a, b, dims=((1,), (0,))):
    def one(left, right):
        return lax.dot_general(left, right, (dims, ((), ())), preferred_element_type=F32)

    (ah, al), (bh, bl) = a, b
    return one(ah, bh) + (one(al, bh) + one(ah, bl))


def part(pos, size):
    return pl.ds(pl.multiple_of(pos * size, size), size)


def added(first, arrived):
    total = first
    for d in range(arrived.shape[0]):
        total = total + arrived[d]
    return total


def kernel(
    f_hbm, v_hbm, t_hbm, out_hbm,
    fv, ft, vown, vsib, tv, th, tl, vh, vl, wh, wl, fin, qp, yr, ys, zr, zs, xr, qf, ut, uin,
    gp, gc, aq, ayr, ays, azr, azs, axr, aqx, gb, bzr, bzs, byr, bys, bxr, gf, gh, gl,
    lsem, ssem, rsem, csem,
):
    row, col = lax.axis_index("row"), lax.axis_index("col")
    at = {"x": col // NC, "y": row // NZ, "z": row % NZ, "c": col % NC}
    x, y, z, c = at.values()
    started = []

    def along(axis, d):
        pos = lax.rem(at[axis] + d, SIZES[axis])
        to = {**at, axis: pos}
        return pos, (to["y"] * NZ + to["z"], to["x"] * NC + to["c"])

    def exchange(axis, source, target):
        sent = []
        for d in range(1, SIZES[axis]):
            pos, peer = along(axis, d)
            index = len(started)
            copy = pltpu.make_async_remote_copy(
                src_ref=source(pos), dst_ref=target(d), send_sem=ssem.at[index], recv_sem=rsem.at[index],
                device_id=peer, device_id_type=MESH,
            )
            copy.start()
            sent.append(copy)
            started.append(copy)
        return sent

    def arrive(sent):
        for copy in sent:
            copy.wait_recv()

    loads = [
        pltpu.make_async_copy(f_hbm, fv, lsem.at[0]),
        pltpu.make_async_copy(t_hbm, tv, lsem.at[1]),
        pltpu.make_async_copy(v_hbm, vown, lsem.at[2]),
    ]
    for load in loads:
        load.start()

    barrier = pltpu.get_barrier_semaphore()
    peers = 0
    for axis, size in SIZES.items():
        for d in range(1, size):
            pl.semaphore_signal(barrier, inc=1, device_id=along(axis, d)[1], device_id_type=MESH)
            peers += 1

    loads[0].wait()

    @pl.loop(0, ROWS // 512)
    def _(b):
        for u in range(4):
            rows = pl.ds(pl.multiple_of(b * 512 + u * 128, 128), 128)
            ft[:, rows] = fv[rows, :].T

    loads[1].wait()
    for k in range(PANELS):
        th[k], tl[k] = split(tv[k].T)
    loads[2].wait()

    def prepare(source, where):
        rows = part(where, OWN)

        @pl.loop(0, PANELS)
        def _(k):
            lanes = part(k, WB)
            v = split(source[k])
            vh[rows, lanes], vl[rows, lanes] = v
            wh[lanes, rows], wl[lanes, rows] = split(dot3((th[k], tl[k]), v, ((1,), (1,))))

    prepare(vown, c)
    mine = part(c, OWN)
    for index, (j, k) in enumerate(PAIRS):
        jl, kl = pl.ds(j * WB, WB), pl.ds(k * WB, WB)
        gp[pl.ds(index * WB, WB), :] = dot3((wh[jl, mine], wl[jl, mine]), (vh[mine, kl], vl[mine, kl]))

    pl.semaphore_wait(barrier, peers)

    copies = {}

    def send_in(h):
        rows = pl.ds(h * CW, CW)
        here = part(x, CW)
        copies["in", h] = exchange("x", lambda pos: ft.at[rows, part(pos, CHIP)], lambda d: fin.at[h, here, :])
        fin[h, here, :] = ft[rows, part(x, CHIP)]

    send_in(0)
    copies["gc"] = exchange("c", lambda pos: gp.at[part(pos, SHARE), :], lambda d: gc)
    copies["sib"] = exchange("c", lambda pos: v_hbm, lambda d: vsib)

    def prepare_sibling():
        arrive(copies["sib"])
        prepare(vsib, 1 - c)

    def stage_in(h):
        arrive(copies["in", h])
        total = dot3(split(fin[h]), (vh[...], vl[...]))
        for k in range(PANELS):
            qp[h, k] = total[:, k * WB : (k + 1) * WB]
        copies["r1", h] = exchange("y", lambda pos: qp.at[h, pos], lambda d: yr.at[h, d - 1])

    def stage_r1(h):
        arrive(copies["r1", h])
        ys[h] = added(qp[h, y], yr.at[h])
        copies["r2", h] = exchange("z", lambda pos: ys.at[h, part(pos, CM // NZ), :], lambda d: zr.at[h, d - 1])

    def stage_r2(h):
        arrive(copies["r2", h])
        zs[h] = added(ys[h, part(z, CM // NZ), :], zr.at[h])
        copies["x", h] = exchange("x", lambda pos: zs.at[h], lambda d: xr.at[h, d - 1])

    def stage_x(h):
        arrive(copies["x", h])
        rows = part(z, CM // NZ)
        qf[h, y, rows, :] = added(zs[h], xr.at[h])
        here = qf.at[h, y, rows, :]
        copies["a1", h] = exchange("z", lambda pos: here, lambda d: here)

    def stage_a1(h):
        arrive(copies["a1", h])
        here = qf.at[h, y]
        copies["a2", h] = exchange("y", lambda pos: here, lambda d: here)

    def stage_out(h):
        arrive(copies["a2", h])
        total = jnp.concatenate([qf[h, k] for k in range(PANELS)], axis=1)
        ut[h] = dot3(split(total), (wh[...], wl[...]))
        rows = pl.ds(h * CW, CW)
        here = part(x, CHIP)
        copies["out", h] = exchange("x", lambda pos: ut.at[h, part(pos, CW), :], lambda d: uin.at[rows, here])
        uin[rows, here] = ut[h, part(x, CW), :]

    def stage_gc():
        arrive(copies["gc"])
        for p in range(NY):
            aq[p] = gp[pl.ds(pl.multiple_of(c * SHARE + p * AM, AM), AM), :] + gc[pl.ds(p * AM, AM), :]
        gb[...] = gp[pl.ds(pl.multiple_of(c * SHARE + HA, HB), HB), :] + gc[pl.ds(HA, HB), :]
        copies["r1", A] = exchange("y", lambda pos: aq.at[pos], lambda d: ayr.at[d - 1])
        copies["b1"] = exchange("z", lambda pos: gb.at[part(pos, BZ), :], lambda d: bzr.at[d - 1])

    def unit(pos):
        return pl.ds(pl.multiple_of(pos // 2 * 8, 8), 8), pl.ds(pl.multiple_of(pos % 2 * 128, 128), 128)

    def pairs_r1():
        arrive(copies["r1", A])
        ays[...] = added(aq[y], ayr)
        copies["r2", A] = exchange("z", lambda pos: ays.at[part(pos, AM // NZ), :], lambda d: azr.at[d - 1])

    def pairs_r2():
        arrive(copies["r2", A])
        azs[...] = added(ays[part(z, AM // NZ), :], azr)
        copies["x", A] = exchange("x", lambda pos: azs.at[*unit(pos)], lambda d: axr.at[d - 1])

    def pairs_x():
        arrive(copies["x", A])
        aqx[x, y, part(z, 8), :] = added(azs[*unit(x)], axr)
        here = aqx.at[x, y, part(z, 8), :]
        copies["a1", A] = exchange("z", lambda pos: here, lambda d: here)

    def pairs_a1():
        arrive(copies["a1", A])
        here = aqx.at[x, y]
        copies["a2", A] = exchange("y", lambda pos: here, lambda d: here)

    def pairs_a2():
        arrive(copies["a2", A])
        here = aqx.at[x]
        copies["a3", A] = exchange("x", lambda pos: here, lambda d: here)

    spot = pl.ds(pl.multiple_of(c * SHARE + HA + z * BZ + y * BY, BY), BY)
    line = pl.ds(pl.multiple_of(c * SHARE + HA + z * BZ, BZ), BZ)

    def stage_b1():
        arrive(copies["b1"])
        bzs[...] = added(gb[part(z, BZ), :], bzr)
        copies["b2"] = exchange("y", lambda pos: bzs.at[part(pos, BY), :], lambda d: byr.at[d - 1])

    def stage_b2():
        arrive(copies["b2"])
        bys[...] = added(bzs[part(y, BY), :], byr)
        copies["b3"] = exchange("x", lambda pos: bys, lambda d: bxr.at[d - 1])

    def stage_b3():
        arrive(copies["b3"])
        gf[spot, :] = added(bys[...], bxr)
        here = gf.at[spot, :]
        copies["b4"] = exchange("y", lambda pos: here, lambda d: here)

    def stage_b4():
        arrive(copies["b4"])
        here = gf.at[line, :]
        copies["b5"] = exchange("z", lambda pos: here, lambda d: here)

    def stage_pairs():
        arrive(copies["a3", A])
        for p in range(NY):
            rows = pl.ds(pl.multiple_of(c * SHARE + p * AM, AM), AM)
            for lane in range(2):
                halves = jnp.stack([aqx[2 * half + lane, p].reshape(NZ, 8, 128) for half in range(2)], 1)
                gf[rows, pl.ds(lane * 128, 128)] = halves.reshape(AM, 128)
        arrive(copies["b5"])
        here = gf.at[part(c, SHARE), :]
        copies["gs"] = exchange("c", lambda pos: here, lambda d: here)

    def fold(j):
        if j == PANELS - 2:
            arrive(copies["gs"])
            gh[...], gl[...] = split(gf[...])
        jl = pl.ds(j * WB, WB)
        total = wh[jl, :].astype(F32) + wl[jl, :].astype(F32)
        for k in range(j + 1, PANELS):
            kl = pl.ds(k * WB, WB)
            pair = pl.ds(PAIRS.index((j, k)) * WB, WB)
            total = total - dot3((gh[pair, :], gl[pair, :]), (wh[kl, :], wl[kl, :]))
        wh[jl, :], wl[jl, :] = split(total)

    stages = {
        "next": send_in, "sib": prepare_sibling, "in": stage_in, "r1": stage_r1, "r2": stage_r2, "x": stage_x,
        "a1": stage_a1, "out": stage_out, "gc": stage_gc, "b1": stage_b1, "b2": stage_b2, "b3": stage_b3, "b4": stage_b4,
        "pairs": stage_pairs, "fold": fold,
    }
    pair_stages = {"r1": pairs_r1, "r2": pairs_r2, "x": pairs_x, "a1": pairs_a1, "a2": pairs_a2}
    for name, *which in ORDER:
        with jax.named_scope("_".join(map(str, [name, *which]))):
            if which == [A]:
                pair_stages[name]()
            else:
                stages[name](*which)

    stores = []

    def finish(pos):
        @pl.loop(0, CHIP // 512)
        def _(b):
            for u in range(4):
                rows = pl.ds(pl.multiple_of(pos * CHIP + b * 512 + u * 128, 128), 128)
                fv[rows, :] = fv[rows, :] - uin[:, rows].T

        store = pltpu.make_async_copy(fv.at[part(pos, CHIP), :], out_hbm.at[part(pos, CHIP), :], csem.at[len(stores)])
        store.start()
        stores.append(store)

    finish(x)
    for d in (1, 3, 2):
        for h in range(CH):
            copies["out", h][d - 1].wait_recv()
        finish(lax.rem(x + NX - d, NX))
    for copy in started:
        copy.wait_send()
    for store in stores:
        store.wait()


COPIES = 2 * (NC - 1) + (NC - 1) + (CH + 1) * (4 * (NX - 1) + 2 * (NY - 1) + 2 * (NZ - 1)) + 2 * (NZ - 1) + 3 * (NX - 1)


def body(eigvecs, reflectors, factors):
    def vm(*shape, dtype=F32):
        return pltpu.VMEM(shape, dtype)

    def half(*shape):
        return [vm(*shape, dtype=BF16)] * 2

    zrows, pairs = CM // NZ, len(PAIRS) * WB
    scratch = [
        vm(ROWS, COLS), vm(COLS, ROWS), vm(PANELS, OWN, WB), vm(PANELS, OWN, WB), vm(PANELS, WB, WB),
        *half(PANELS, WB, WB), *half(CHIP, WIDE), *half(WIDE, CHIP),
        vm(CH, CM, CHIP), vm(CH, PANELS, CM, WB), vm(CH, NY - 1, CM, WB), vm(CH, CM, WB), vm(CH, NZ - 1, zrows, WB),
        vm(CH, zrows, WB), vm(CH, NX - 1, zrows, WB), vm(CH, PANELS, CM, WB), vm(CH, CM, CHIP), vm(COLS, ROWS),
        vm(pairs, WB), vm(SHARE, WB), vm(NY, AM, WB), vm(NY - 1, AM, WB), vm(AM, WB), vm(NZ - 1, AM // NZ, WB),
        vm(AM // NZ, WB), vm(NX - 1, 8, 128), vm(NX, NY, NZ * 8, 128),
        vm(HB, WB), vm(NZ - 1, BZ, WB), vm(BZ, WB), vm(NY - 1, BY, WB), vm(BY, WB), vm(NX - 1, BY, WB),
        vm(pairs, WB), *half(pairs, WB),
        pltpu.SemaphoreType.DMA((3,)), pltpu.SemaphoreType.DMA((COPIES,)), pltpu.SemaphoreType.DMA((COPIES,)),
        pltpu.SemaphoreType.DMA((NX,)),
    ]
    return pl.pallas_call(
        kernel,
        out_shape=jax.ShapeDtypeStruct((ROWS, COLS), F32),
        in_specs=[pl.BlockSpec(memory_space=pl.ANY)] * 3,
        out_specs=pl.BlockSpec(memory_space=pl.ANY),
        scratch_shapes=scratch,
        compiler_params=pltpu.CompilerParams(collective_id=0, has_side_effects=True, vmem_limit_bytes=63 * 2**20),
        name="back_transform",
    )(eigvecs, reflectors, factors)


def solution(mesh):
    in_specs = (P("row", "col"), P(None, ("row", "col"), None), P())
    return jax.shard_map(body, mesh=mesh, in_specs=in_specs, out_specs=P("row", "col"), check_vma=False)
```

```python
import jax
import jax.numpy as jnp
from jax import lax
from jax.experimental import pallas as pl
from jax.experimental.pallas import tpu as pltpu
from jax.sharding import PartitionSpec as P

MESH = pl.DeviceIdType.MESH
F32 = jnp.float32
BF16 = jnp.bfloat16

SIZES = {"x": 4, "y": 4, "z": 8, "c": 2}
NX, NY, NZ, NC = SIZES.values()
PANELS, WB = 4, 256
ROWS, COLS = 4096, 128
OWN = 512
CHIP = NC * OWN
WIDE = PANELS * WB
CH = 8
CW = COLS // CH
CM = NX * CW
PAIRS = [(0, 1), (0, 2), (0, 3), (1, 2), (1, 3), (2, 3)]
SHARE = len(PAIRS) // NC * WB
HA = 2 * WB
HB = SHARE - HA
AM = HA // NY
BZ, BY = HB // NZ, HB // NZ // NY
A = CH
ORDER = [
    ("next", 1), ("next", 2), ("next", 3), ("next", 4), ("gc",), ("sib",), ("in", 0), ("in", 1), ("r1", A), ("in", 2), ("b1",),
    ("r1", 0), ("in", 3), ("next", 5), ("r1", 1), ("in", 4), ("r2", A), ("b2",), ("r1", 2), ("r2", 0), ("next", 6), ("next", 7),
    ("x", A), ("b3",), ("r1", 3), ("in", 5), ("x", 0), ("r2", 1), ("r1", 4), ("a1", A), ("r2", 2), ("b4",), ("in", 6), ("in", 7),
    ("r2", 3), ("x", 1), ("a1", 0), ("a2", A), ("r1", 5), ("r1", 6), ("x", 2), ("r2", 4), ("b5",), ("r1", 7), ("x", 3), ("a1", 1),
    ("fold", 2), ("r2", 5), ("pairs",), ("r2", 6), ("x", 4), ("fold", 1), ("x", 5), ("a1", 2), ("fold", 0), ("out", 0), ("r2", 7),
    ("x", 6), ("a1", 3), ("out", 1), ("a1", 4), ("out", 2), ("a1", 6), ("x", 7), ("a1", 5), ("out", 3), ("out", 4), ("a1", 7),
    ("out", 6), ("out", 5), ("out", 7),
]


def split(x):
    high = x.astype(BF16)
    return high, (x - high.astype(F32)).astype(BF16)


def dot3(a, b, dims=((1,), (0,))):
    def one(left, right):
        return lax.dot_general(left, right, (dims, ((), ())), preferred_element_type=F32)

    (ah, al), (bh, bl) = a, b
    rows = ah.shape[0]
    both = one(jnp.concatenate([ah, al], axis=0), bh)
    return both[:rows] + (both[rows:] + one(ah, bl))


def part(pos, size):
    return pl.ds(pl.multiple_of(pos * size, size), size)


def added(first, arrived):
    total = first
    for d in range(arrived.shape[0]):
        total = total + arrived[d]
    return total


def kernel(
    f_hbm, v_hbm, t_hbm, out_hbm,
    fv, ft, vown, vsib, tv, th, tl, vh, vl, wh, wl, fin, qp, yr, ys, zr, zs, xr, qf, ut, uin,
    gp, gc, aq, ayr, ays, azr, azs, axr, aqx, gb, bzr, bzs, byr, bys, bxr, gf,
    lsem, ssem, rsem, csem,
):
    row, col = lax.axis_index("row"), lax.axis_index("col")
    at = {"x": col // NC, "y": row // NZ, "z": row % NZ, "c": col % NC}
    x, y, z, c = at.values()

    def along(axis, d):
        pos = lax.rem(at[axis] + d, SIZES[axis])
        to = {**at, axis: pos}
        return pos, (to["y"] * NZ + to["z"], to["x"] * NC + to["c"])

    sends = {}
    arrivals = [0]

    def exchange(axis, source, target, whole, kind=None, recv=None):
        slot = sends.setdefault(kind or ("only", len(sends)), (len(sends), whole))[0]
        if recv is None:
            recv = [arrivals[0]] * SIZES[axis]
            arrivals[0] += 1
        for d in range(1, SIZES[axis]):
            pos, peer = along(axis, d)
            pltpu.make_async_remote_copy(
                src_ref=source(pos), dst_ref=target(d), send_sem=ssem.at[slot], recv_sem=rsem.at[recv[d]],
                device_id=peer, device_id_type=MESH,
            ).start()
        return recv[1], whole

    def arrive(sent):
        pltpu.make_async_copy(sent[1], sent[1], rsem.at[sent[0]]).wait()

    loads = [
        pltpu.make_async_copy(t_hbm, tv, lsem.at[1]),
        pltpu.make_async_copy(v_hbm, vown, lsem.at[2]),
        pltpu.make_async_copy(f_hbm, fv, lsem.at[0]),
    ]
    for load in loads:
        load.start()

    barrier = pltpu.get_barrier_semaphore()
    peers = 0
    for axis, size in SIZES.items():
        for d in range(1, size):
            pl.semaphore_signal(barrier, inc=1, device_id=along(axis, d)[1], device_id_type=MESH)
            peers += 1

    loads[0].wait()
    for k in range(PANELS):
        th[k], tl[k] = split(tv[k].T)
    loads[1].wait()

    def prepare(source, where):
        rows = part(where, OWN)

        @pl.loop(0, PANELS)
        def _(k):
            lanes = part(k, WB)
            v = split(source[k])
            vh[rows, lanes], vl[rows, lanes] = v
            wh[lanes, rows], wl[lanes, rows] = split(dot3((th[k], tl[k]), v, ((1,), (1,))))

    prepare(vown, c)
    mine = part(c, OWN)
    for index, (j, k) in enumerate(PAIRS):
        jl, kl = pl.ds(j * WB, WB), pl.ds(k * WB, WB)
        gp[pl.ds(index * WB, WB), :] = dot3((wh[jl, mine], wl[jl, mine]), (vh[mine, kl], vl[mine, kl]))

    pl.semaphore_wait(barrier, peers)

    copies = {}
    back = [None, 0, 1, 2]
    arrivals[0] = NX - 1
    copies["gc"] = exchange("c", lambda pos: gp.at[part(pos, SHARE), :], lambda d: gc, gc)
    copies["sib"] = exchange("c", lambda pos: v_hbm, lambda d: vsib, vsib)

    loads[2].wait()

    @pl.loop(0, ROWS // 512)
    def _(b):
        for u in range(4):
            rows = pl.ds(pl.multiple_of(b * 512 + u * 128, 128), 128)
            ft[:, rows] = fv[rows, :].T


    def send_in(h):
        rows = pl.ds(h * CW, CW)
        here = part(x, CW)
        copies["in", h] = exchange("x", lambda pos: ft.at[rows, part(pos, CHIP)], lambda d: fin.at[h, here, :], fin.at[h, pl.ds(0, CM - CW), :], "in")
        fin[h, here, :] = ft[rows, part(x, CHIP)]

    send_in(0)

    def prepare_sibling():
        arrive(copies["sib"])
        prepare(vsib, 1 - c)

    def stage_in(h):
        arrive(copies["in", h])
        total = dot3(split(fin[h]), (vh[...], vl[...]))
        for k in range(PANELS):
            qp[h, k] = total[:, k * WB : (k + 1) * WB]
        copies["r1", h] = exchange("y", lambda pos: qp.at[h, pos], lambda d: yr.at[h, d - 1], yr.at[h], "r1")

    def stage_r1(h):
        arrive(copies["r1", h])
        ys[h] = added(qp[h, y], yr.at[h])
        copies["r2", h] = exchange("z", lambda pos: ys.at[h, part(pos, CM // NZ), :], lambda d: zr.at[h, d - 1], zr.at[h], "r2")

    def stage_r2(h):
        arrive(copies["r2", h])
        zs[h] = added(ys[h, part(z, CM // NZ), :], zr.at[h])
        copies["x", h] = exchange("x", lambda pos: zs.at[h], lambda d: xr.at[h, d - 1], xr.at[h], "x")

    def stage_x(h):
        arrive(copies["x", h])
        rows = part(z, CM // NZ)
        qf[h, y, rows, :] = added(zs[h], xr.at[h])
        here = qf.at[h, y, rows, :]
        copies["a1", h] = exchange("z", lambda pos: here, lambda d: here, zr.at[h], "a1")

    def stage_a1(h):
        arrive(copies["a1", h])
        here = qf.at[h, y]
        copies["a2", h] = exchange("y", lambda pos: here, lambda d: here, yr.at[h], "a2")

    def stage_out(h):
        arrive(copies["a2", h])
        total = jnp.concatenate([qf[h, k] for k in range(PANELS)], axis=1)
        ut[h] = dot3(split(total), (wh[...], wl[...]))
        rows = pl.ds(h * CW, CW)
        here = part(x, CHIP)
        exchange("x", lambda pos: ut.at[h, part(pos, CW), :], lambda d: uin.at[rows, here], None, "out", back)
        uin[rows, here] = ut[h, part(x, CW), :]

    def stage_gc():
        arrive(copies["gc"])
        for p in range(NY):
            aq[p] = gp[pl.ds(pl.multiple_of(c * SHARE + p * AM, AM), AM), :] + gc[pl.ds(p * AM, AM), :]
        gb[...] = gp[pl.ds(pl.multiple_of(c * SHARE + HA, HB), HB), :] + gc[pl.ds(HA, HB), :]
        copies["r1", A] = exchange("y", lambda pos: aq.at[pos], lambda d: ayr.at[d - 1], ayr)
        copies["b1"] = exchange("z", lambda pos: gb.at[part(pos, BZ), :], lambda d: bzr.at[d - 1], bzr)

    def unit(pos):
        return pl.ds(pl.multiple_of(pos // 2 * 8, 8), 8), pl.ds(pl.multiple_of(pos % 2 * 128, 128), 128)

    def pairs_r1():
        arrive(copies["r1", A])
        ays[...] = added(aq[y], ayr)
        copies["r2", A] = exchange("z", lambda pos: ays.at[part(pos, AM // NZ), :], lambda d: azr.at[d - 1], azr)

    def pairs_r2():
        arrive(copies["r2", A])
        azs[...] = added(ays[part(z, AM // NZ), :], azr)
        copies["x", A] = exchange("x", lambda pos: azs.at[*unit(pos)], lambda d: axr.at[d - 1], axr)

    def pairs_x():
        arrive(copies["x", A])
        aqx[x, y, part(z, 8), :] = added(azs[*unit(x)], axr)
        here = aqx.at[x, y, part(z, 8), :]
        copies["a1", A] = exchange("z", lambda pos: here, lambda d: here, aqx.at[x, y, pl.ds(0, 8 * (NZ - 1)), :])

    def pairs_a1():
        arrive(copies["a1", A])
        here = aqx.at[x, y]
        copies["a2", A] = exchange("y", lambda pos: here, lambda d: here, aqx.at[x, pl.ds(0, NY - 1)])

    def pairs_a2():
        arrive(copies["a2", A])
        here = aqx.at[x]
        copies["a3", A] = exchange("x", lambda pos: here, lambda d: here, aqx.at[pl.ds(0, NX - 1)])

    spot = pl.ds(pl.multiple_of(c * SHARE + HA + z * BZ + y * BY, BY), BY)
    line = pl.ds(pl.multiple_of(c * SHARE + HA + z * BZ, BZ), BZ)

    def stage_b1():
        arrive(copies["b1"])
        bzs[...] = added(gb[part(z, BZ), :], bzr)
        copies["b2"] = exchange("y", lambda pos: bzs.at[part(pos, BY), :], lambda d: byr.at[d - 1], byr)

    def stage_b2():
        arrive(copies["b2"])
        bys[...] = added(bzs[part(y, BY), :], byr)
        copies["b3"] = exchange("x", lambda pos: bys, lambda d: bxr.at[d - 1], bxr)

    def stage_b3():
        arrive(copies["b3"])
        gf[spot, :] = added(bys[...], bxr)
        here = gf.at[spot, :]
        copies["b4"] = exchange("y", lambda pos: here, lambda d: here, byr)

    def stage_b4():
        arrive(copies["b4"])
        here = gf.at[line, :]
        copies["b5"] = exchange("z", lambda pos: here, lambda d: here, bzr)

    def stage_pairs():
        arrive(copies["a3", A])
        for p in range(NY):
            rows = pl.ds(pl.multiple_of(c * SHARE + p * AM, AM), AM)
            for lane in range(2):
                halves = jnp.stack([aqx[2 * half + lane, p].reshape(NZ, 8, 128) for half in range(2)], 1)
                gf[rows, pl.ds(lane * 128, 128)] = halves.reshape(AM, 128)
        here = gf.at[pl.ds(pl.multiple_of(c * SHARE, HB), HA), :]
        copies["gs"] = exchange("c", lambda pos: here, lambda d: here, here)

    def stage_b5():
        arrive(copies["b5"])
        here = gf.at[pl.ds(pl.multiple_of(c * SHARE + HA, HB), HB), :]
        copies["b6"] = exchange("c", lambda pos: here, lambda d: here, here)

    def fold(j):
        terms = {2: [(2, 3), (0, 3)], 1: [(1, 2), (1, 3)], 0: [(0, 1), (0, 2)]}[j]
        if j == 2:
            arrive(copies["b6"])
        if j == 1:
            arrive(copies["gs"])
        for target in sorted({term[0] for term in terms}):
            lines = pl.ds(target * WB, WB)
            total = wh[lines, :].astype(F32) + wl[lines, :].astype(F32)
            for k in [term[1] for term in terms if term[0] == target]:
                kl = pl.ds(k * WB, WB)
                pair = pl.ds(PAIRS.index((target, k)) * WB, WB)
                total = total - dot3(split(gf[pair, :]), (wh[kl, :], wl[kl, :]))
            wh[lines, :], wl[lines, :] = split(total)

    stages = {
        "next": send_in, "sib": prepare_sibling, "in": stage_in, "r1": stage_r1, "r2": stage_r2, "x": stage_x,
        "a1": stage_a1, "out": stage_out, "gc": stage_gc, "b1": stage_b1, "b2": stage_b2, "b3": stage_b3, "b4": stage_b4,
        "b5": stage_b5, "pairs": stage_pairs, "fold": fold,
    }
    pair_stages = {"r1": pairs_r1, "r2": pairs_r2, "x": pairs_x, "a1": pairs_a1, "a2": pairs_a2}
    for name, *which in ORDER:
        with jax.named_scope("_".join(map(str, [name, *which]))):
            if which == [A]:
                pair_stages[name]()
            else:
                stages[name](*which)

    stores = []

    def finish(pos):
        @pl.loop(0, CHIP // 512)
        def _(b):
            for u in range(4):
                rows = pl.ds(pl.multiple_of(pos * CHIP + b * 512 + u * 128, 128), 128)
                fv[rows, :] = fv[rows, :] - uin[:, rows].T

        store = pltpu.make_async_copy(fv.at[part(pos, CHIP), :], out_hbm.at[part(pos, CHIP), :], csem.at[len(stores)])
        store.start()
        stores.append(store)

    finish(x)
    for d in (1, 3, 2):
        pos = lax.rem(x + NX - d, NX)
        arrive((back[d], uin.at[:, part(pos, CHIP)]))
        finish(pos)
    all_in = fin.at[pl.ds(0, CH * (NX - 1) // NX)]
    totals = {"in": all_in, "out": all_in, "r1": yr, "r2": zr, "x": xr, "a1": zr, "a2": yr}
    for kind, (slot, whole) in sends.items():
        sent = totals.get(kind, whole)
        pltpu.make_async_copy(sent, sent, ssem.at[slot]).wait()
    for store in stores:
        store.wait()


SENDS, ARRIVALS = 22, NX - 1 + 6 * CH + 15


def body(eigvecs, reflectors, factors):
    def vm(*shape, dtype=F32):
        return pltpu.VMEM(shape, dtype)

    def half(*shape):
        return [vm(*shape, dtype=BF16)] * 2

    zrows, pairs = CM // NZ, len(PAIRS) * WB
    scratch = [
        vm(ROWS, COLS), vm(COLS, ROWS), vm(PANELS, OWN, WB), vm(PANELS, OWN, WB), vm(PANELS, WB, WB),
        *half(PANELS, WB, WB), *half(CHIP, WIDE), *half(WIDE, CHIP),
        vm(CH, CM, CHIP), vm(CH, PANELS, CM, WB), vm(CH, NY - 1, CM, WB), vm(CH, CM, WB), vm(CH, NZ - 1, zrows, WB),
        vm(CH, zrows, WB), vm(CH, NX - 1, zrows, WB), vm(CH, PANELS, CM, WB), vm(CH, CM, CHIP), vm(COLS, ROWS),
        vm(pairs, WB), vm(SHARE, WB), vm(NY, AM, WB), vm(NY - 1, AM, WB), vm(AM, WB), vm(NZ - 1, AM // NZ, WB),
        vm(AM // NZ, WB), vm(NX - 1, 8, 128), vm(NX, NY, NZ * 8, 128),
        vm(HB, WB), vm(NZ - 1, BZ, WB), vm(BZ, WB), vm(NY - 1, BY, WB), vm(BY, WB), vm(NX - 1, BY, WB),
        vm(pairs, WB),
        pltpu.SemaphoreType.DMA((3,)), pltpu.SemaphoreType.DMA((SENDS,)), pltpu.SemaphoreType.DMA((ARRIVALS,)),
        pltpu.SemaphoreType.DMA((NX,)),
    ]
    return pl.pallas_call(
        kernel,
        out_shape=jax.ShapeDtypeStruct((ROWS, COLS), F32),
        in_specs=[pl.BlockSpec(memory_space=pl.ANY)] * 3,
        out_specs=pl.BlockSpec(memory_space=pl.ANY),
        scratch_shapes=scratch,
        compiler_params=pltpu.CompilerParams(collective_id=0, has_side_effects=True, vmem_limit_bytes=63 * 2**20),
        name="back_transform",
    )(eigvecs, reflectors, factors)


def solution(mesh):
    in_specs = (P("row", "col"), P(None, ("row", "col"), None), P())
    return jax.shard_map(body, mesh=mesh, in_specs=in_specs, out_specs=P("row", "col"), check_vma=False)
```

```python
import jax
import jax.numpy as jnp
from jax import lax
from jax.experimental import pallas as pl
from jax.experimental.pallas import tpu as pltpu
from jax.sharding import PartitionSpec as P

MESH = pl.DeviceIdType.MESH
F32 = jnp.float32
BF16 = jnp.bfloat16

SIZES = {"x": 4, "y": 4, "z": 8, "c": 2}
NX, NY, NZ, NC = SIZES.values()
PANELS, WB = 4, 256
ROWS, COLS = 4096, 128
OWN = 512
CHIP = NC * OWN
WIDE = PANELS * WB
CH = 8
CW = COLS // CH
CM = NX * CW
PAIRS = [(0, 1), (0, 2), (0, 3), (1, 2), (1, 3), (2, 3)]
SHARE = len(PAIRS) // NC * WB
HA = 2 * WB
HB = SHARE - HA
AM = HA // NY
BZ, BY = HB // NZ, HB // NZ // NY
A = CH
ORDER = [
    ("next", 1), ("next", 2), ("next", 3), ("next", 4), ("gc",), ("sib",), ("in", 0), ("in", 1), ("r1", A), ("in", 2), ("b1",),
    ("r1", 0), ("in", 3), ("next", 5), ("r1", 1), ("in", 4), ("r2", A), ("b2",), ("r1", 2), ("r2", 0), ("next", 6), ("next", 7),
    ("x", A), ("b3",), ("r1", 3), ("in", 5), ("x", 0), ("r2", 1), ("r1", 4), ("a1", A), ("r2", 2), ("b4",), ("in", 6), ("in", 7),
    ("r2", 3), ("x", 1), ("a1", 0), ("a2", A), ("r1", 5), ("r1", 6), ("x", 2), ("r2", 4), ("b5",), ("r1", 7), ("x", 3), ("a1", 1),
    ("fold", 2), ("r2", 5), ("pairs",), ("r2", 6), ("x", 4), ("fold", 1), ("x", 5), ("a1", 2), ("fold", 0), ("out", 0), ("r2", 7),
    ("x", 6), ("a1", 3), ("out", 1), ("a1", 4), ("out", 2), ("a1", 6), ("x", 7), ("a1", 5), ("out", 3), ("out", 4), ("a1", 7),
    ("out", 6), ("out", 5), ("out", 7),
]


def split(x):
    high = x.astype(BF16)
    return high, (x - high.astype(F32)).astype(BF16)


def dot3(a, b, dims=((1,), (0,))):
    def one(left, right):
        return lax.dot_general(left, right, (dims, ((), ())), preferred_element_type=F32)

    (ah, al), (bh, bl) = a, b
    rows = ah.shape[0]
    both = one(jnp.concatenate([ah, al], axis=0), bh)
    return both[:rows] + (both[rows:] + one(ah, bl))


def part(pos, size):
    return pl.ds(pl.multiple_of(pos * size, size), size)


def added(first, arrived):
    total = first
    for d in range(arrived.shape[0]):
        total = total + arrived[d]
    return total


def kernel(
    f_hbm, v_hbm, t_hbm, out_hbm,
    fv, ft, vown, vsib, tv, th, tl, vh, vl, wh, wl, fin, qp, yr, ys, zr, zs, xr, qf, ut, uin,
    gp, gc, aq, ayr, ays, azr, azs, axr, aqx, gb, bzr, bzs, byr, bys, bxr, gf,
    lsem, ssem, rsem, csem,
):
    row, col = lax.axis_index("row"), lax.axis_index("col")
    at = {"x": col // NC, "y": row // NZ, "z": row % NZ, "c": col % NC}
    x, y, z, c = at.values()

    def along(axis, d):
        pos = lax.rem(at[axis] + d, SIZES[axis])
        to = {**at, axis: pos}
        return pos, (to["y"] * NZ + to["z"], to["x"] * NC + to["c"])

    sends = {}
    arrivals = [0]

    def exchange(axis, source, target, whole, kind=None, recv=None):
        slot = sends.setdefault(kind or ("only", len(sends)), (len(sends), whole))[0]
        if recv is None:
            recv = [arrivals[0]] * SIZES[axis]
            arrivals[0] += 1
        for d in range(1, SIZES[axis]):
            pos, peer = along(axis, d)
            pltpu.make_async_remote_copy(
                src_ref=source(pos), dst_ref=target(d), send_sem=ssem.at[slot], recv_sem=rsem.at[recv[d]],
                device_id=peer, device_id_type=MESH,
            ).start()
        return recv[1], whole

    def arrive(sent):
        pltpu.make_async_copy(sent[1], sent[1], rsem.at[sent[0]]).wait()

    loads = [
        pltpu.make_async_copy(t_hbm, tv, lsem.at[1]),
        pltpu.make_async_copy(v_hbm, vown, lsem.at[2]),
        pltpu.make_async_copy(f_hbm, fv, lsem.at[0]),
    ]
    for load in loads:
        load.start()

    barrier = pltpu.get_barrier_semaphore()
    peers = 0
    for axis, size in SIZES.items():
        for d in range(1, size):
            pl.semaphore_signal(barrier, inc=1, device_id=along(axis, d)[1], device_id_type=MESH)
            peers += 1

    loads[0].wait()
    for k in range(PANELS):
        th[k], tl[k] = split(tv[k].T)
    loads[1].wait()

    def prepare(source, where):
        rows = part(where, OWN)

        @pl.loop(0, PANELS)
        def _(k):
            lanes = part(k, WB)
            v = split(source[k])
            vh[rows, lanes], vl[rows, lanes] = v
            wh[lanes, rows], wl[lanes, rows] = split(dot3((th[k], tl[k]), v, ((1,), (1,))))

    prepare(vown, c)
    mine = part(c, OWN)
    for index, (j, k) in enumerate(PAIRS):
        jl, kl = pl.ds(j * WB, WB), pl.ds(k * WB, WB)
        gp[pl.ds(index * WB, WB), :] = dot3((wh[jl, mine], wl[jl, mine]), (vh[mine, kl], vl[mine, kl]))

    pl.semaphore_wait(barrier, peers)

    copies = {}
    back = [None, 0, 1, 2]
    arrivals[0] = NX - 1
    copies["gc"] = exchange("c", lambda pos: gp.at[part(pos, SHARE), :], lambda d: gc, gc)
    copies["sib"] = exchange("c", lambda pos: v_hbm, lambda d: vsib, vsib)

    loads[2].wait()

    @pl.loop(0, ROWS // 512)
    def _(b):
        for u in range(4):
            rows = pl.ds(pl.multiple_of(b * 512 + u * 128, 128), 128)
            ft[:, rows] = fv[rows, :].T


    def send_in(h):
        rows = pl.ds(h * CW, CW)
        here = part(x, CW)
        copies["in", h] = exchange("x", lambda pos: ft.at[rows, part(pos, CHIP)], lambda d: fin.at[h, here, :], fin.at[h, pl.ds(0, CM - CW), :], "in")
        fin[h, here, :] = ft[rows, part(x, CHIP)]

    send_in(0)

    def prepare_sibling():
        arrive(copies["sib"])
        prepare(vsib, 1 - c)

    def stage_in(h):
        arrive(copies["in", h])
        total = dot3(split(fin[h]), (vh[...], vl[...]))
        for k in range(PANELS):
            qp[h, k] = total[:, k * WB : (k + 1) * WB]
        copies["r1", h] = exchange("y", lambda pos: qp.at[h, pos], lambda d: yr.at[h, d - 1], yr.at[h], "r1")

    def stage_r1(h):
        arrive(copies["r1", h])
        ys[h] = added(qp[h, y], yr.at[h])
        copies["r2", h] = exchange("z", lambda pos: ys.at[h, part(pos, CM // NZ), :], lambda d: zr.at[h, d - 1], zr.at[h], "r2")

    def stage_r2(h):
        arrive(copies["r2", h])
        zs[h] = added(ys[h, part(z, CM // NZ), :], zr.at[h])
        copies["x", h] = exchange("x", lambda pos: zs.at[h], lambda d: xr.at[h, d - 1], xr.at[h], "x")

    def stage_x(h):
        arrive(copies["x", h])
        rows = part(z, CM // NZ)
        qf[h, y, rows, :] = added(zs[h], xr.at[h])
        here = qf.at[h, y, rows, :]
        copies["a1", h] = exchange("z", lambda pos: here, lambda d: here, zr.at[h], "a1")

    def stage_a1(h):
        arrive(copies["a1", h])
        here = qf.at[h, y]
        copies["a2", h] = exchange("y", lambda pos: here, lambda d: here, yr.at[h], "a2")

    def stage_out(h):
        arrive(copies["a2", h])
        total = jnp.concatenate([qf[h, k] for k in range(PANELS)], axis=1)
        ut[h] = dot3(split(total), (wh[...], wl[...]))
        rows = pl.ds(h * CW, CW)
        here = part(x, CHIP)
        exchange("x", lambda pos: ut.at[h, part(pos, CW), :], lambda d: uin.at[rows, here], None, "out", back)
        uin[rows, here] = ut[h, part(x, CW), :]

    def stage_gc():
        arrive(copies["gc"])
        for p in range(NY):
            aq[p] = gp[pl.ds(pl.multiple_of(c * SHARE + p * AM, AM), AM), :] + gc[pl.ds(p * AM, AM), :]
        gb[...] = gp[pl.ds(pl.multiple_of(c * SHARE + HA, HB), HB), :] + gc[pl.ds(HA, HB), :]
        copies["r1", A] = exchange("y", lambda pos: aq.at[pos], lambda d: ayr.at[d - 1], ayr)
        copies["b1"] = exchange("z", lambda pos: gb.at[part(pos, BZ), :], lambda d: bzr.at[d - 1], bzr)

    def unit(pos):
        return pl.ds(pl.multiple_of(pos // 2 * 8, 8), 8), pl.ds(pl.multiple_of(pos % 2 * 128, 128), 128)

    def pairs_r1():
        arrive(copies["r1", A])
        ays[...] = added(aq[y], ayr)
        copies["r2", A] = exchange("z", lambda pos: ays.at[part(pos, AM // NZ), :], lambda d: azr.at[d - 1], azr)

    def pairs_r2():
        arrive(copies["r2", A])
        azs[...] = added(ays[part(z, AM // NZ), :], azr)
        copies["x", A] = exchange("x", lambda pos: azs.at[*unit(pos)], lambda d: axr.at[d - 1], axr)

    def pairs_x():
        arrive(copies["x", A])
        aqx[x, y, part(z, 8), :] = added(azs[*unit(x)], axr)
        here = aqx.at[x, y, part(z, 8), :]
        copies["a1", A] = exchange("z", lambda pos: here, lambda d: here, aqx.at[x, y, pl.ds(0, 8 * (NZ - 1)), :])

    def pairs_a1():
        arrive(copies["a1", A])
        here = aqx.at[x, y]
        copies["a2", A] = exchange("y", lambda pos: here, lambda d: here, aqx.at[x, pl.ds(0, NY - 1)])

    def pairs_a2():
        arrive(copies["a2", A])
        here = aqx.at[x]
        copies["a3", A] = exchange("x", lambda pos: here, lambda d: here, aqx.at[pl.ds(0, NX - 1)])

    spot = pl.ds(pl.multiple_of(c * SHARE + HA + z * BZ + y * BY, BY), BY)
    line = pl.ds(pl.multiple_of(c * SHARE + HA + z * BZ, BZ), BZ)

    def stage_b1():
        arrive(copies["b1"])
        bzs[...] = added(gb[part(z, BZ), :], bzr)
        copies["b2"] = exchange("y", lambda pos: bzs.at[part(pos, BY), :], lambda d: byr.at[d - 1], byr)

    def stage_b2():
        arrive(copies["b2"])
        bys[...] = added(bzs[part(y, BY), :], byr)
        copies["b3"] = exchange("x", lambda pos: bys, lambda d: bxr.at[d - 1], bxr)

    def stage_b3():
        arrive(copies["b3"])
        gf[spot, :] = added(bys[...], bxr)
        here = gf.at[spot, :]
        copies["b4"] = exchange("y", lambda pos: here, lambda d: here, byr)

    def stage_b4():
        arrive(copies["b4"])
        here = gf.at[line, :]
        copies["b5"] = exchange("z", lambda pos: here, lambda d: here, bzr)

    def stage_pairs():
        arrive(copies["a3", A])
        for p in range(NY):
            rows = pl.ds(pl.multiple_of(c * SHARE + p * AM, AM), AM)
            for lane in range(2):
                halves = jnp.stack([aqx[2 * half + lane, p].reshape(NZ, 8, 128) for half in range(2)], 1)
                gf[rows, pl.ds(lane * 128, 128)] = halves.reshape(AM, 128)
        here = gf.at[pl.ds(pl.multiple_of(c * SHARE, HB), HA), :]
        copies["gs"] = exchange("c", lambda pos: here, lambda d: here, here)

    def stage_b5():
        arrive(copies["b5"])
        here = gf.at[pl.ds(pl.multiple_of(c * SHARE + HA, HB), HB), :]
        copies["b6"] = exchange("c", lambda pos: here, lambda d: here, here)

    def fold(j):
        terms = {2: [(2, 3), (0, 3)], 1: [(1, 2), (1, 3)], 0: [(0, 1), (0, 2)]}[j]
        if j == 2:
            arrive(copies["b6"])
        if j == 1:
            arrive(copies["gs"])
        for target in sorted({term[0] for term in terms}):
            lines = pl.ds(target * WB, WB)
            total = wh[lines, :].astype(F32) + wl[lines, :].astype(F32)
            for k in [term[1] for term in terms if term[0] == target]:
                kl = pl.ds(k * WB, WB)
                pair = pl.ds(PAIRS.index((target, k)) * WB, WB)
                total = total - dot3(split(gf[pair, :]), (wh[kl, :], wl[kl, :]))
            wh[lines, :], wl[lines, :] = split(total)

    stages = {
        "next": send_in, "sib": prepare_sibling, "in": stage_in, "r1": stage_r1, "r2": stage_r2, "x": stage_x,
        "a1": stage_a1, "out": stage_out, "gc": stage_gc, "b1": stage_b1, "b2": stage_b2, "b3": stage_b3, "b4": stage_b4,
        "b5": stage_b5, "pairs": stage_pairs, "fold": fold,
    }
    pair_stages = {"r1": pairs_r1, "r2": pairs_r2, "x": pairs_x, "a1": pairs_a1, "a2": pairs_a2}
    for name, *which in ORDER:
        with jax.named_scope("_".join(map(str, [name, *which]))):
            if which == [A]:
                pair_stages[name]()
            else:
                stages[name](*which)

    stores = []

    def finish(pos):
        @pl.loop(0, CHIP // 512)
        def _(b):
            for u in range(4):
                rows = pl.ds(pl.multiple_of(pos * CHIP + b * 512 + u * 128, 128), 128)
                fv[rows, :] = fv[rows, :] - uin[:, rows].T

        store = pltpu.make_async_copy(fv.at[part(pos, CHIP), :], out_hbm.at[part(pos, CHIP), :], csem.at[len(stores)])
        store.start()
        stores.append(store)

    finish(x)
    for d in (1, 3, 2):
        pos = lax.rem(x + NX - d, NX)
        arrive((back[d], uin.at[:, part(pos, CHIP)]))
        finish(pos)
    all_in = fin.at[pl.ds(0, CH * (NX - 1) // NX)]
    totals = {"in": all_in, "out": all_in, "r1": yr, "r2": zr, "x": xr, "a1": zr, "a2": yr}
    for kind, (slot, whole) in sends.items():
        sent = totals.get(kind, whole)
        pltpu.make_async_copy(sent, sent, ssem.at[slot]).wait()
    for store in stores:
        store.wait()


SENDS, ARRIVALS = 22, NX - 1 + 6 * CH + 15


def body(eigvecs, reflectors, factors):
    def vm(*shape, dtype=F32):
        return pltpu.VMEM(shape, dtype)

    def half(*shape):
        return [vm(*shape, dtype=BF16)] * 2

    zrows, pairs = CM // NZ, len(PAIRS) * WB
    scratch = [
        vm(ROWS, COLS), vm(COLS, ROWS), vm(PANELS, OWN, WB), vm(PANELS, OWN, WB), vm(PANELS, WB, WB),
        *half(PANELS, WB, WB), *half(CHIP, WIDE), *half(WIDE, CHIP),
        vm(CH, CM, CHIP), vm(CH, PANELS, CM, WB), vm(CH, NY - 1, CM, WB), vm(CH, CM, WB), vm(CH, NZ - 1, zrows, WB),
        vm(CH, zrows, WB), vm(CH, NX - 1, zrows, WB), vm(CH, PANELS, CM, WB), vm(CH, CM, CHIP), vm(COLS, ROWS),
        vm(pairs, WB), vm(SHARE, WB), vm(NY, AM, WB), vm(NY - 1, AM, WB), vm(AM, WB), vm(NZ - 1, AM // NZ, WB),
        vm(AM // NZ, WB), vm(NX - 1, 8, 128), vm(NX, NY, NZ * 8, 128),
        vm(HB, WB), vm(NZ - 1, BZ, WB), vm(BZ, WB), vm(NY - 1, BY, WB), vm(BY, WB), vm(NX - 1, BY, WB),
        vm(pairs, WB),
        pltpu.SemaphoreType.DMA((3,)), pltpu.SemaphoreType.DMA((SENDS,)), pltpu.SemaphoreType.DMA((ARRIVALS,)),
        pltpu.SemaphoreType.DMA((NX,)),
    ]
    return pl.pallas_call(
        kernel,
        out_shape=jax.ShapeDtypeStruct((ROWS, COLS), F32),
        in_specs=[pl.BlockSpec(memory_space=pl.ANY)] * 3,
        out_specs=pl.BlockSpec(memory_space=pl.ANY),
        scratch_shapes=scratch,
        compiler_params=pltpu.CompilerParams(collective_id=0, has_side_effects=True, vmem_limit_bytes=49 * 2**20),
        name="back_transform",
    )(eigvecs, reflectors, factors)


def solution(mesh):
    in_specs = (P("row", "col"), P(None, ("row", "col"), None), P())
    return jax.shard_map(body, mesh=mesh, in_specs=in_specs, out_specs=P("row", "col"), check_vma=False)
```

```python
import jax
import jax.numpy as jnp
from jax import lax
from jax.experimental import pallas as pl
from jax.experimental.pallas import tpu as pltpu
from jax.sharding import PartitionSpec as P

MESH = pl.DeviceIdType.MESH
F32 = jnp.float32
BF16 = jnp.bfloat16

SIZES = {"x": 4, "y": 4, "z": 8, "c": 2}
NX, NY, NZ, NC = SIZES.values()
PANELS, WB = 4, 256
ROWS, COLS = 4096, 128
OWN = 512
CHIP = NC * OWN
WIDE = PANELS * WB
CH = 8
CW = COLS // CH
CM = NX * CW
PAIRS = [(0, 1), (0, 2), (0, 3), (1, 2), (1, 3), (2, 3)]
SHARE = len(PAIRS) // NC * WB
HA = 2 * WB
HB = SHARE - HA
AM = HA // NY
BZ, BY = HB // NZ, HB // NZ // NY
A = CH
ORDER = [
    ("next", 1), ("gc",), ("next", 2), ("sib",), ("next", 3), ("in", 0), ("next", 4), ("in", 1), ("b1",), ("r1", A), ("next", 5),
    ("in", 2), ("r1", 0), ("in", 4), ("r2", A), ("b2",), ("r1", 1), ("r2", 0), ("next", 6), ("x", A), ("b3",), ("r1", 2),
    ("x", 0), ("in", 5), ("r2", 1), ("r1", 4), ("next", 7), ("b4",), ("a1", A), ("x", 1), ("in", 3), ("r2", 2), ("in", 6),
    ("in", 7), ("r2", 4), ("r1", 5), ("a2", A), ("a1", 0), ("x", 2), ("r1", 3), ("b5",), ("r1", 6), ("x", 4), ("a1", 1),
    ("r2", 5), ("pairs",), ("fold", 2), ("r1", 7), ("a1", 2), ("fold", 1), ("r2", 3), ("x", 5), ("fold", 0), ("r2", 6),
    ("out", 0), ("a1", 4), ("x", 3), ("r2", 7), ("out", 1), ("a1", 5), ("x", 6), ("out", 2), ("x", 7), ("a1", 3), ("out", 4),
    ("a1", 6), ("a1", 7), ("out", 5), ("out", 3), ("out", 6), ("out", 7),
]


def split(x):
    high = x.astype(BF16)
    return high, (x - high.astype(F32)).astype(BF16)


def dot3(a, b, dims=((1,), (0,))):
    def one(left, right):
        return lax.dot_general(left, right, (dims, ((), ())), preferred_element_type=F32)

    (ah, al), (bh, bl) = a, b
    rows = ah.shape[0]
    both = one(jnp.concatenate([ah, al], axis=0), bh)
    return both[:rows] + (both[rows:] + one(ah, bl))


def part(pos, size):
    return pl.ds(pl.multiple_of(pos * size, size), size)


def added(first, arrived):
    total = first
    for d in range(arrived.shape[0]):
        total = total + arrived[d]
    return total


def kernel(
    f_hbm, v_hbm, t_hbm, out_hbm,
    fv, ft, vown, vsib, tv, th, tl, vh, vl, wh, wl, fin, qp, yr, ys, zr, zs, xr, qf, ut, uin,
    gp, gc, aq, ayr, ays, azr, azs, axr, aqx, gb, bzr, bzs, byr, bys, bxr, gf,
    lsem, ssem, rsem, csem,
):
    row, col = lax.axis_index("row"), lax.axis_index("col")
    at = {"x": col // NC, "y": row // NZ, "z": row % NZ, "c": col % NC}
    x, y, z, c = at.values()

    def along(axis, d):
        pos = lax.rem(at[axis] + d, SIZES[axis])
        to = {**at, axis: pos}
        return pos, (to["y"] * NZ + to["z"], to["x"] * NC + to["c"])

    sends = {}
    arrivals = [0]

    def exchange(axis, source, target, whole, kind=None, recv=None):
        slot = sends.setdefault(kind or ("only", len(sends)), (len(sends), whole))[0]
        if recv is None:
            recv = [arrivals[0]] * SIZES[axis]
            arrivals[0] += 1
        for d in sorted(range(1, SIZES[axis]), key=lambda d: -min(d, SIZES[axis] - d)):
            pos, peer = along(axis, d)
            pltpu.make_async_remote_copy(
                src_ref=source(pos), dst_ref=target(d), send_sem=ssem.at[slot], recv_sem=rsem.at[recv[d]],
                device_id=peer, device_id_type=MESH,
            ).start()
        return recv[1], whole

    def arrive(sent):
        pltpu.make_async_copy(sent[1], sent[1], rsem.at[sent[0]]).wait()

    loads = [
        pltpu.make_async_copy(t_hbm, tv, lsem.at[1]),
        pltpu.make_async_copy(v_hbm, vown, lsem.at[2]),
        pltpu.make_async_copy(f_hbm, fv, lsem.at[0]),
    ]
    for load in loads:
        load.start()

    barrier = pltpu.get_barrier_semaphore()
    peers = 0
    for axis, size in SIZES.items():
        for d in range(1, size):
            pl.semaphore_signal(barrier, inc=1, device_id=along(axis, d)[1], device_id_type=MESH)
            peers += 1

    loads[0].wait()
    for k in range(PANELS):
        th[k], tl[k] = split(tv[k].T)
    loads[1].wait()

    def prepare(source, where):
        rows = part(where, OWN)

        @pl.loop(0, PANELS)
        def _(k):
            lanes = part(k, WB)
            v = split(source[k])
            vh[rows, lanes], vl[rows, lanes] = v
            wh[lanes, rows], wl[lanes, rows] = split(dot3((th[k], tl[k]), v, ((1,), (1,))))

    prepare(vown, c)
    mine = part(c, OWN)
    for index, (j, k) in enumerate(PAIRS):
        jl, kl = pl.ds(j * WB, WB), pl.ds(k * WB, WB)
        gp[pl.ds(index * WB, WB), :] = dot3((wh[jl, mine], wl[jl, mine]), (vh[mine, kl], vl[mine, kl]))

    pl.semaphore_wait(barrier, peers)

    copies = {}
    back = [None, 0, 1, 2]
    arrivals[0] = NX - 1
    copies["gc"] = exchange("c", lambda pos: gp.at[part(pos, SHARE), :], lambda d: gc, gc)
    copies["sib"] = exchange("c", lambda pos: v_hbm, lambda d: vsib, vsib)

    loads[2].wait()

    @pl.loop(0, ROWS // 512)
    def _(b):
        for u in range(4):
            rows = pl.ds(pl.multiple_of(b * 512 + u * 128, 128), 128)
            ft[:, rows] = fv[rows, :].T


    def send_in(h):
        rows = pl.ds(h * CW, CW)
        here = part(x, CW)
        copies["in", h] = exchange("x", lambda pos: ft.at[rows, part(pos, CHIP)], lambda d: fin.at[h, here, :], fin.at[h, pl.ds(0, CM - CW), :], "in")
        fin[h, here, :] = ft[rows, part(x, CHIP)]

    send_in(0)

    def prepare_sibling():
        arrive(copies["sib"])
        prepare(vsib, 1 - c)

    def stage_in(h):
        arrive(copies["in", h])
        total = dot3(split(fin[h]), (vh[...], vl[...]))
        for k in range(PANELS):
            qp[h, k] = total[:, k * WB : (k + 1) * WB]
        copies["r1", h] = exchange("y", lambda pos: qp.at[h, pos], lambda d: yr.at[h, d - 1], yr.at[h], "r1")

    def stage_r1(h):
        arrive(copies["r1", h])
        ys[h] = added(qp[h, y], yr.at[h])
        copies["r2", h] = exchange("z", lambda pos: ys.at[h, part(pos, CM // NZ), :], lambda d: zr.at[h, d - 1], zr.at[h], "r2")

    def stage_r2(h):
        arrive(copies["r2", h])
        zs[h] = added(ys[h, part(z, CM // NZ), :], zr.at[h])
        copies["x", h] = exchange("x", lambda pos: zs.at[h], lambda d: xr.at[h, d - 1], xr.at[h], "x")

    def stage_x(h):
        arrive(copies["x", h])
        rows = part(z, CM // NZ)
        qf[h, y, rows, :] = added(zs[h], xr.at[h])
        here = qf.at[h, y, rows, :]
        copies["a1", h] = exchange("z", lambda pos: here, lambda d: here, zr.at[h], "a1")

    def stage_a1(h):
        arrive(copies["a1", h])
        here = qf.at[h, y]
        copies["a2", h] = exchange("y", lambda pos: here, lambda d: here, yr.at[h], "a2")

    def stage_out(h):
        arrive(copies["a2", h])
        total = jnp.concatenate([qf[h, k] for k in range(PANELS)], axis=1)
        ut[h] = dot3(split(total), (wh[...], wl[...]))
        rows = pl.ds(h * CW, CW)
        here = part(x, CHIP)
        exchange("x", lambda pos: ut.at[h, part(pos, CW), :], lambda d: uin.at[rows, here], None, "out", back)
        uin[rows, here] = ut[h, part(x, CW), :]

    def stage_gc():
        arrive(copies["gc"])
        for p in range(NY):
            aq[p] = gp[pl.ds(pl.multiple_of(c * SHARE + p * AM, AM), AM), :] + gc[pl.ds(p * AM, AM), :]
        gb[...] = gp[pl.ds(pl.multiple_of(c * SHARE + HA, HB), HB), :] + gc[pl.ds(HA, HB), :]
        copies["r1", A] = exchange("y", lambda pos: aq.at[pos], lambda d: ayr.at[d - 1], ayr)
        copies["b1"] = exchange("z", lambda pos: gb.at[part(pos, BZ), :], lambda d: bzr.at[d - 1], bzr)

    def unit(pos):
        return pl.ds(pl.multiple_of(pos // 2 * 8, 8), 8), pl.ds(pl.multiple_of(pos % 2 * 128, 128), 128)

    def pairs_r1():
        arrive(copies["r1", A])
        ays[...] = added(aq[y], ayr)
        copies["r2", A] = exchange("z", lambda pos: ays.at[part(pos, AM // NZ), :], lambda d: azr.at[d - 1], azr)

    def pairs_r2():
        arrive(copies["r2", A])
        azs[...] = added(ays[part(z, AM // NZ), :], azr)
        copies["x", A] = exchange("x", lambda pos: azs.at[*unit(pos)], lambda d: axr.at[d - 1], axr)

    def pairs_x():
        arrive(copies["x", A])
        aqx[x, y, part(z, 8), :] = added(azs[*unit(x)], axr)
        here = aqx.at[x, y, part(z, 8), :]
        copies["a1", A] = exchange("z", lambda pos: here, lambda d: here, aqx.at[x, y, pl.ds(0, 8 * (NZ - 1)), :])

    def pairs_a1():
        arrive(copies["a1", A])
        here = aqx.at[x, y]
        copies["a2", A] = exchange("y", lambda pos: here, lambda d: here, aqx.at[x, pl.ds(0, NY - 1)])

    def pairs_a2():
        arrive(copies["a2", A])
        here = aqx.at[x]
        copies["a3", A] = exchange("x", lambda pos: here, lambda d: here, aqx.at[pl.ds(0, NX - 1)])

    spot = pl.ds(pl.multiple_of(c * SHARE + HA + z * BZ + y * BY, BY), BY)
    line = pl.ds(pl.multiple_of(c * SHARE + HA + z * BZ, BZ), BZ)

    def stage_b1():
        arrive(copies["b1"])
        bzs[...] = added(gb[part(z, BZ), :], bzr)
        copies["b2"] = exchange("y", lambda pos: bzs.at[part(pos, BY), :], lambda d: byr.at[d - 1], byr)

    def stage_b2():
        arrive(copies["b2"])
        bys[...] = added(bzs[part(y, BY), :], byr)
        copies["b3"] = exchange("x", lambda pos: bys, lambda d: bxr.at[d - 1], bxr)

    def stage_b3():
        arrive(copies["b3"])
        gf[spot, :] = added(bys[...], bxr)
        here = gf.at[spot, :]
        copies["b4"] = exchange("y", lambda pos: here, lambda d: here, byr)

    def stage_b4():
        arrive(copies["b4"])
        here = gf.at[line, :]
        copies["b5"] = exchange("z", lambda pos: here, lambda d: here, bzr)

    def stage_pairs():
        arrive(copies["a3", A])
        for p in range(NY):
            rows = pl.ds(pl.multiple_of(c * SHARE + p * AM, AM), AM)
            for lane in range(2):
                halves = jnp.stack([aqx[2 * half + lane, p].reshape(NZ, 8, 128) for half in range(2)], 1)
                gf[rows, pl.ds(lane * 128, 128)] = halves.reshape(AM, 128)
        here = gf.at[pl.ds(pl.multiple_of(c * SHARE, HB), HA), :]
        copies["gs"] = exchange("c", lambda pos: here, lambda d: here, here)

    def stage_b5():
        arrive(copies["b5"])
        here = gf.at[pl.ds(pl.multiple_of(c * SHARE + HA, HB), HB), :]
        copies["b6"] = exchange("c", lambda pos: here, lambda d: here, here)

    def fold(j):
        if j:
            arrive(copies["b6" if j == 2 else "gs"])
        for target, first, last in {2: [(2, 3, 3), (0, 3, 3)], 1: [(1, 2, 3)], 0: [(0, 1, 2)]}[j]:
            lines, others = pl.ds(target * WB, WB), pl.ds(first * WB, (last + 1 - first) * WB)
            blocks = [gf[pl.ds(PAIRS.index((target, k)) * WB, WB), :] for k in range(first, last + 1)]
            total = wh[lines, :].astype(F32) + wl[lines, :].astype(F32)
            taken = dot3(split(jnp.concatenate(blocks, axis=1)), (wh[others, :], wl[others, :]))
            wh[lines, :], wl[lines, :] = split(total - taken)

    stages = {
        "next": send_in, "sib": prepare_sibling, "in": stage_in, "r1": stage_r1, "r2": stage_r2, "x": stage_x,
        "a1": stage_a1, "out": stage_out, "gc": stage_gc, "b1": stage_b1, "b2": stage_b2, "b3": stage_b3, "b4": stage_b4,
        "b5": stage_b5, "pairs": stage_pairs, "fold": fold,
    }
    pair_stages = {"r1": pairs_r1, "r2": pairs_r2, "x": pairs_x, "a1": pairs_a1, "a2": pairs_a2}
    for name, *which in ORDER:
        with jax.named_scope("_".join(map(str, [name, *which]))):
            if which == [A]:
                pair_stages[name]()
            else:
                stages[name](*which)

    stores = []

    def finish(pos):
        @pl.loop(0, CHIP // 512)
        def _(b):
            for u in range(4):
                rows = pl.ds(pl.multiple_of(pos * CHIP + b * 512 + u * 128, 128), 128)
                fv[rows, :] = fv[rows, :] - uin[:, rows].T

        store = pltpu.make_async_copy(fv.at[part(pos, CHIP), :], out_hbm.at[part(pos, CHIP), :], csem.at[len(stores)])
        store.start()
        stores.append(store)

    finish(x)
    for d in (1, 3, 2):
        pos = lax.rem(x + NX - d, NX)
        arrive((back[d], uin.at[:, part(pos, CHIP)]))
        finish(pos)
    all_in = fin.at[pl.ds(0, CH * (NX - 1) // NX)]
    totals = {"in": all_in, "out": all_in, "r1": yr, "r2": zr, "x": xr, "a1": zr, "a2": yr}
    for kind, (slot, whole) in sends.items():
        sent = totals.get(kind, whole)
        pltpu.make_async_copy(sent, sent, ssem.at[slot]).wait()
    for store in stores:
        store.wait()


SENDS, ARRIVALS = 22, NX - 1 + 6 * CH + 15


def body(eigvecs, reflectors, factors):
    def vm(*shape, dtype=F32):
        return pltpu.VMEM(shape, dtype)

    def half(*shape):
        return [vm(*shape, dtype=BF16)] * 2

    zrows, pairs = CM // NZ, len(PAIRS) * WB
    scratch = [
        vm(ROWS, COLS), vm(COLS, ROWS), vm(PANELS, OWN, WB), vm(PANELS, OWN, WB), vm(PANELS, WB, WB),
        *half(PANELS, WB, WB), *half(CHIP, WIDE), *half(WIDE, CHIP),
        vm(CH, CM, CHIP), vm(CH, PANELS, CM, WB), vm(CH, NY - 1, CM, WB), vm(CH, CM, WB), vm(CH, NZ - 1, zrows, WB),
        vm(CH, zrows, WB), vm(CH, NX - 1, zrows, WB), vm(CH, PANELS, CM, WB), vm(CH, CM, CHIP), vm(COLS, ROWS),
        vm(pairs, WB), vm(SHARE, WB), vm(NY, AM, WB), vm(NY - 1, AM, WB), vm(AM, WB), vm(NZ - 1, AM // NZ, WB),
        vm(AM // NZ, WB), vm(NX - 1, 8, 128), vm(NX, NY, NZ * 8, 128),
        vm(HB, WB), vm(NZ - 1, BZ, WB), vm(BZ, WB), vm(NY - 1, BY, WB), vm(BY, WB), vm(NX - 1, BY, WB),
        vm(pairs, WB),
        pltpu.SemaphoreType.DMA((3,)), pltpu.SemaphoreType.DMA((SENDS,)), pltpu.SemaphoreType.DMA((ARRIVALS,)),
        pltpu.SemaphoreType.DMA((NX,)),
    ]
    return pl.pallas_call(
        kernel,
        out_shape=jax.ShapeDtypeStruct((ROWS, COLS), F32),
        in_specs=[pl.BlockSpec(memory_space=pl.ANY)] * 3,
        out_specs=pl.BlockSpec(memory_space=pl.ANY),
        scratch_shapes=scratch,
        compiler_params=pltpu.CompilerParams(collective_id=0, has_side_effects=True, vmem_limit_bytes=49 * 2**20),
        name="back_transform",
    )(eigvecs, reflectors, factors)


def solution(mesh):
    in_specs = (P("row", "col"), P(None, ("row", "col"), None), P())
    return jax.shard_map(body, mesh=mesh, in_specs=in_specs, out_specs=P("row", "col"), check_vma=False)
```

```python
import jax
import jax.numpy as jnp
from jax import lax
from jax.experimental import pallas as pl
from jax.experimental.pallas import tpu as pltpu
from jax.sharding import PartitionSpec as P

MESH = pl.DeviceIdType.MESH
F32 = jnp.float32
BF16 = jnp.bfloat16

SIZES = {"x": 4, "y": 4, "z": 8, "c": 2}
NX, NY, NZ, NC = SIZES.values()
PANELS, WB = 4, 256
ROWS, COLS = 4096, 128
OWN = 512
CHIP = NC * OWN
WIDE = PANELS * WB
CH = 8
CW = COLS // CH
CM = NX * CW
PAIRS = [(0, 1), (0, 2), (0, 3), (1, 2), (1, 3), (2, 3)]
SHARE = len(PAIRS) // NC * WB
HA = 2 * WB
HB = SHARE - HA
AM = HA // NY
BZ, BY = HB // NZ, HB // NZ // NY
A = CH
ORDER = [
    ("next", 1), ("gc",), ("next", 2), ("sib",), ("next", 3), ("in", 0), ("next", 4), ("in", 1), ("b1",), ("r1", A), ("next", 5),
    ("in", 2), ("r1", 0), ("in", 4), ("r2", A), ("b2",), ("r1", 1), ("r2", 0), ("next", 6), ("x", A), ("b3",), ("r1", 2),
    ("x", 0), ("in", 5), ("r2", 1), ("r1", 4), ("next", 7), ("b4",), ("a1", A), ("x", 1), ("in", 3), ("r2", 2), ("in", 6),
    ("in", 7), ("r2", 4), ("r1", 5), ("a2", A), ("a1", 0), ("x", 2), ("r1", 3), ("b5",), ("r1", 6), ("x", 4), ("a1", 1),
    ("r2", 5), ("pairs",), ("fold", 2), ("r1", 7), ("a1", 2), ("fold", 1), ("r2", 3), ("x", 5), ("fold", 0), ("r2", 6),
    ("out", 0), ("a1", 4), ("x", 3), ("r2", 7), ("out", 1), ("a1", 5), ("x", 6), ("out", 2), ("x", 7), ("a1", 3), ("out", 4),
    ("a1", 6), ("a1", 7), ("out", 5), ("out", 3), ("out", 6), ("out", 7),
]


def split(x):
    high = x.astype(BF16)
    return high, (x - high.astype(F32)).astype(BF16)


def dot3(a, b, dims=((1,), (0,))):
    def one(left, right):
        return lax.dot_general(left, right, (dims, ((), ())), preferred_element_type=F32)

    (ah, al), (bh, bl) = a, b
    rows = ah.shape[0]
    both = one(jnp.concatenate([ah, al], axis=0), bh)
    return both[:rows] + (both[rows:] + one(ah, bl))


def part(pos, size):
    return pl.ds(pl.multiple_of(pos * size, size), size)


def added(first, arrived):
    total = first
    for d in range(arrived.shape[0]):
        total = total + arrived[d]
    return total


def kernel(
    f_hbm, v_hbm, t_hbm, out_hbm,
    fv, ft, vown, vsib, tv, th, tl, vh, vl, wh, wl, fin, qp, yr, ys, zr, zs, xr, qf, ut, uin,
    gp, gc, aq, ayr, ays, azr, azs, axr, aqx, gb, bzr, bzs, byr, bys, bxr, gf,
    lsem, ssem, rsem, csem,
):
    row, col = lax.axis_index("row"), lax.axis_index("col")
    at = {"x": col // NC, "y": row // NZ, "z": row % NZ, "c": col % NC}
    x, y, z, c = at.values()

    def along(axis, d):
        pos = lax.rem(at[axis] + d, SIZES[axis])
        to = {**at, axis: pos}
        return pos, (to["y"] * NZ + to["z"], to["x"] * NC + to["c"])

    sends = {}
    arrivals = [0]

    def exchange(axis, source, target, whole, kind=None, recv=None):
        slot = sends.setdefault(kind or ("only", len(sends)), (len(sends), whole))[0]
        if recv is None:
            recv = [arrivals[0]] * SIZES[axis]
            arrivals[0] += 1
        for d in sorted(range(1, SIZES[axis]), key=lambda d: -min(d, SIZES[axis] - d)):
            pos, peer = along(axis, d)
            pltpu.make_async_remote_copy(
                src_ref=source(pos), dst_ref=target(d), send_sem=ssem.at[slot], recv_sem=rsem.at[recv[d]],
                device_id=peer, device_id_type=MESH,
            ).start()
        return recv[1], whole

    def arrive(sent):
        pltpu.make_async_copy(sent[1], sent[1], rsem.at[sent[0]]).wait()

    loads = [
        pltpu.make_async_copy(t_hbm, tv, lsem.at[1]),
        pltpu.make_async_copy(v_hbm, vown, lsem.at[2]),
        pltpu.make_async_copy(f_hbm, fv, lsem.at[0]),
    ]
    for load in loads:
        load.start()

    barrier = pltpu.get_barrier_semaphore()
    peers = 0
    for axis, size in SIZES.items():
        for d in range(1, size):
            pl.semaphore_signal(barrier, inc=1, device_id=along(axis, d)[1], device_id_type=MESH)
            peers += 1

    loads[0].wait()
    for k in range(PANELS):
        th[k], tl[k] = split(tv[k].T)
    loads[1].wait()

    def prepare(source, where):
        rows = part(where, OWN)

        @pl.loop(0, PANELS)
        def _(k):
            lanes = part(k, WB)
            v = split(source[k])
            vh[rows, lanes], vl[rows, lanes] = v
            wh[lanes, rows], wl[lanes, rows] = split(dot3((th[k], tl[k]), v, ((1,), (1,))))

    prepare(vown, c)
    mine = part(c, OWN)
    for index, (j, k) in enumerate(PAIRS):
        jl, kl = pl.ds(j * WB, WB), pl.ds(k * WB, WB)
        gp[pl.ds(index * WB, WB), :] = dot3((wh[jl, mine], wl[jl, mine]), (vh[mine, kl], vl[mine, kl]))

    pl.semaphore_wait(barrier, peers)

    copies = {}
    back = [None, 0, 1, 2]
    arrivals[0] = NX - 1
    copies["gc"] = exchange("c", lambda pos: gp.at[part(pos, SHARE), :], lambda d: gc, gc)
    copies["sib"] = exchange("c", lambda pos: v_hbm, lambda d: vsib, vsib)

    loads[2].wait()

    @pl.loop(0, ROWS // 512)
    def _(b):
        for u in range(4):
            rows = pl.ds(pl.multiple_of(b * 512 + u * 128, 128), 128)
            ft[:, rows] = fv[rows, :].T


    def send_in(h):
        rows = pl.ds(h * CW, CW)
        here = part(x, CW)
        copies["in", h] = exchange("x", lambda pos: ft.at[rows, part(pos, CHIP)], lambda d: fin.at[h, here, :], fin.at[h, pl.ds(0, CM - CW), :], "in")
        fin[h, here, :] = ft[rows, part(x, CHIP)]

    send_in(0)

    def prepare_sibling():
        arrive(copies["sib"])
        prepare(vsib, 1 - c)

    def stage_in(h):
        arrive(copies["in", h])
        total = dot3(split(fin[h]), (vh[...], vl[...]))
        for k in range(PANELS):
            qp[h, k] = total[:, k * WB : (k + 1) * WB]
        copies["r1", h] = exchange("y", lambda pos: qp.at[h, pos], lambda d: yr.at[h, d - 1], yr.at[h], "r1")

    def stage_r1(h):
        arrive(copies["r1", h])
        ys[h] = added(qp[h, y], yr.at[h])
        copies["r2", h] = exchange("z", lambda pos: ys.at[h, part(pos, CM // NZ), :], lambda d: zr.at[h, d - 1], zr.at[h], "r2")

    def stage_r2(h):
        arrive(copies["r2", h])
        zs[h] = added(ys[h, part(z, CM // NZ), :], zr.at[h])
        copies["x", h] = exchange("x", lambda pos: zs.at[h], lambda d: xr.at[h, d - 1], xr.at[h], "x")

    def stage_x(h):
        arrive(copies["x", h])
        rows = part(z, CM // NZ)
        qf[h, y, rows, :] = added(zs[h], xr.at[h])
        here = qf.at[h, y, rows, :]
        copies["a1", h] = exchange("z", lambda pos: here, lambda d: here, zr.at[h], "a1")

    def stage_a1(h):
        arrive(copies["a1", h])
        here = qf.at[h, y]
        copies["a2", h] = exchange("y", lambda pos: here, lambda d: here, yr.at[h], "a2")

    def stage_out(h):
        arrive(copies["a2", h])
        total = jnp.concatenate([qf[h, k] for k in range(PANELS)], axis=1)
        ut[h] = dot3(split(total), (wh[...], wl[...]))
        rows = pl.ds(h * CW, CW)
        here = part(x, CHIP)
        exchange("x", lambda pos: ut.at[h, part(pos, CW), :], lambda d: uin.at[rows, here], None, "out", back)
        uin[rows, here] = ut[h, part(x, CW), :]

    def stage_gc():
        arrive(copies["gc"])
        for p in range(NY):
            aq[p] = gp[pl.ds(pl.multiple_of(c * SHARE + p * AM, AM), AM), :] + gc[pl.ds(p * AM, AM), :]
        gb[...] = gp[pl.ds(pl.multiple_of(c * SHARE + HA, HB), HB), :] + gc[pl.ds(HA, HB), :]
        copies["r1", A] = exchange("y", lambda pos: aq.at[pos], lambda d: ayr.at[d - 1], ayr)
        copies["b1"] = exchange("z", lambda pos: gb.at[part(pos, BZ), :], lambda d: bzr.at[d - 1], bzr)

    def unit(pos):
        return pl.ds(pl.multiple_of(pos // 2 * 8, 8), 8), pl.ds(pl.multiple_of(pos % 2 * 128, 128), 128)

    def pairs_r1():
        arrive(copies["r1", A])
        ays[...] = added(aq[y], ayr)
        copies["r2", A] = exchange("z", lambda pos: ays.at[part(pos, AM // NZ), :], lambda d: azr.at[d - 1], azr)

    def pairs_r2():
        arrive(copies["r2", A])
        azs[...] = added(ays[part(z, AM // NZ), :], azr)
        copies["x", A] = exchange("x", lambda pos: azs.at[*unit(pos)], lambda d: axr.at[d - 1], axr)

    def pairs_x():
        arrive(copies["x", A])
        aqx[x, y, part(z, 8), :] = added(azs[*unit(x)], axr)
        here = aqx.at[x, y, part(z, 8), :]
        copies["a1", A] = exchange("z", lambda pos: here, lambda d: here, aqx.at[x, y, pl.ds(0, 8 * (NZ - 1)), :])

    def pairs_a1():
        arrive(copies["a1", A])
        here = aqx.at[x, y]
        copies["a2", A] = exchange("y", lambda pos: here, lambda d: here, aqx.at[x, pl.ds(0, NY - 1)])

    def pairs_a2():
        arrive(copies["a2", A])
        here = aqx.at[x]
        copies["a3", A] = exchange("x", lambda pos: here, lambda d: here, aqx.at[pl.ds(0, NX - 1)])

    spot = pl.ds(pl.multiple_of(c * SHARE + HA + z * BZ + y * BY, BY), BY)
    line = pl.ds(pl.multiple_of(c * SHARE + HA + z * BZ, BZ), BZ)

    def stage_b1():
        arrive(copies["b1"])
        bzs[...] = added(gb[part(z, BZ), :], bzr)
        copies["b2"] = exchange("y", lambda pos: bzs.at[part(pos, BY), :], lambda d: byr.at[d - 1], byr)

    def stage_b2():
        arrive(copies["b2"])
        bys[...] = added(bzs[part(y, BY), :], byr)
        copies["b3"] = exchange("x", lambda pos: bys, lambda d: bxr.at[d - 1], bxr)

    def stage_b3():
        arrive(copies["b3"])
        gf[spot, :] = added(bys[...], bxr)
        here = gf.at[spot, :]
        copies["b4"] = exchange("y", lambda pos: here, lambda d: here, byr)

    def stage_b4():
        arrive(copies["b4"])
        here = gf.at[line, :]
        copies["b5"] = exchange("z", lambda pos: here, lambda d: here, bzr)

    def stage_pairs():
        arrive(copies["a3", A])
        for p in range(NY):
            rows = pl.ds(pl.multiple_of(c * SHARE + p * AM, AM), AM)
            for lane in range(2):
                halves = jnp.stack([aqx[2 * half + lane, p].reshape(NZ, 8, 128) for half in range(2)], 1)
                gf[rows, pl.ds(lane * 128, 128)] = halves.reshape(AM, 128)
        here = gf.at[pl.ds(pl.multiple_of(c * SHARE, HB), HA), :]
        copies["gs"] = exchange("c", lambda pos: here, lambda d: here, here)

    def stage_b5():
        arrive(copies["b5"])
        here = gf.at[pl.ds(pl.multiple_of(c * SHARE + HA, HB), HB), :]
        copies["b6"] = exchange("c", lambda pos: here, lambda d: here, here)

    def fold(j):
        if j:
            arrive(copies["b6" if j == 2 else "gs"])
        for target, first, last in {2: [(2, 3, 3), (0, 3, 3)], 1: [(1, 2, 3)], 0: [(0, 1, 2)]}[j]:
            lines, others = pl.ds(target * WB, WB), pl.ds(first * WB, (last + 1 - first) * WB)
            blocks = [gf[pl.ds(PAIRS.index((target, k)) * WB, WB), :] for k in range(first, last + 1)]
            total = wh[lines, :].astype(F32) + wl[lines, :].astype(F32)
            taken = dot3(split(jnp.concatenate(blocks, axis=1)), (wh[others, :], wl[others, :]))
            wh[lines, :], wl[lines, :] = split(total - taken)

    stages = {
        "next": send_in, "sib": prepare_sibling, "in": stage_in, "r1": stage_r1, "r2": stage_r2, "x": stage_x,
        "a1": stage_a1, "out": stage_out, "gc": stage_gc, "b1": stage_b1, "b2": stage_b2, "b3": stage_b3, "b4": stage_b4,
        "b5": stage_b5, "pairs": stage_pairs, "fold": fold,
    }
    pair_stages = {"r1": pairs_r1, "r2": pairs_r2, "x": pairs_x, "a1": pairs_a1, "a2": pairs_a2}
    for name, *which in ORDER:
        with jax.named_scope("_".join(map(str, [name, *which]))):
            if which == [A]:
                pair_stages[name]()
            else:
                stages[name](*which)

    stores = []

    def finish(pos):
        @pl.loop(0, CHIP // 512)
        def _(b):
            for u in range(4):
                rows = pl.ds(pl.multiple_of(pos * CHIP + b * 512 + u * 128, 128), 128)
                fv[rows, :] = fv[rows, :] - uin[:, rows].T

        store = pltpu.make_async_copy(fv.at[part(pos, CHIP), :], out_hbm.at[part(pos, CHIP), :], csem.at[len(stores)])
        store.start()
        stores.append(store)

    finish(x)
    for d in (2, 1, 3):
        pos = lax.rem(x + NX - d, NX)
        arrive((back[d], uin.at[:, part(pos, CHIP)]))
        finish(pos)
    all_in = fin.at[pl.ds(0, CH * (NX - 1) // NX)]
    totals = {"in": all_in, "out": all_in, "r1": yr, "r2": zr, "x": xr, "a1": zr, "a2": yr}
    for kind, (slot, whole) in sends.items():
        sent = totals.get(kind, whole)
        pltpu.make_async_copy(sent, sent, ssem.at[slot]).wait()
    for store in stores:
        store.wait()


SENDS, ARRIVALS = 22, NX - 1 + 6 * CH + 15


def body(eigvecs, reflectors, factors):
    def vm(*shape, dtype=F32):
        return pltpu.VMEM(shape, dtype)

    def half(*shape):
        return [vm(*shape, dtype=BF16)] * 2

    zrows, pairs = CM // NZ, len(PAIRS) * WB
    scratch = [
        vm(ROWS, COLS), vm(COLS, ROWS), vm(PANELS, OWN, WB), vm(PANELS, OWN, WB), vm(PANELS, WB, WB),
        *half(PANELS, WB, WB), *half(CHIP, WIDE), *half(WIDE, CHIP),
        vm(CH, CM, CHIP), vm(CH, PANELS, CM, WB), vm(CH, NY - 1, CM, WB), vm(CH, CM, WB), vm(CH, NZ - 1, zrows, WB),
        vm(CH, zrows, WB), vm(CH, NX - 1, zrows, WB), vm(CH, PANELS, CM, WB), vm(CH, CM, CHIP), vm(COLS, ROWS),
        vm(pairs, WB), vm(SHARE, WB), vm(NY, AM, WB), vm(NY - 1, AM, WB), vm(AM, WB), vm(NZ - 1, AM // NZ, WB),
        vm(AM // NZ, WB), vm(NX - 1, 8, 128), vm(NX, NY, NZ * 8, 128),
        vm(HB, WB), vm(NZ - 1, BZ, WB), vm(BZ, WB), vm(NY - 1, BY, WB), vm(BY, WB), vm(NX - 1, BY, WB),
        vm(pairs, WB),
        pltpu.SemaphoreType.DMA((3,)), pltpu.SemaphoreType.DMA((SENDS,)), pltpu.SemaphoreType.DMA((ARRIVALS,)),
        pltpu.SemaphoreType.DMA((NX,)),
    ]
    return pl.pallas_call(
        kernel,
        out_shape=jax.ShapeDtypeStruct((ROWS, COLS), F32),
        in_specs=[pl.BlockSpec(memory_space=pl.ANY)] * 3,
        out_specs=pl.BlockSpec(memory_space=pl.ANY),
        scratch_shapes=scratch,
        compiler_params=pltpu.CompilerParams(collective_id=0, has_side_effects=True, vmem_limit_bytes=49 * 2**20),
        name="back_transform",
    )(eigvecs, reflectors, factors)


def solution(mesh):
    in_specs = (P("row", "col"), P(None, ("row", "col"), None), P())
    return jax.shard_map(body, mesh=mesh, in_specs=in_specs, out_specs=P("row", "col"), check_vma=False)
```
